16 devices in a mesh: dp: 2 (over y, z), tp: 8 (over x, core).
Axes of the slice: x: 4, y: 2, z: 1, core: 2. Of those that a mesh axis runs over, the one named last changes fastest.
The devices are a block of a 4x4x8 slice.
Arguments:
- x: bfloat16 [24, 256, 5120], P('dp', 'tp'), parts along dimension 0
- k_cache: bfloat16 [24, 1024, 8, 128], P('dp', None, 'tp'), parts along dimension 0
- v_cache: bfloat16 [24, 1024, 8, 128], P('dp', None, 'tp'), parts along dimension 0
- prefix_len: int32 [24], P('dp'), parts along dimension 0
- valid_len: int32 [24], P('dp'), parts along dimension 0
- g_attn: bfloat16 [5120], replicated
- w_q: bfloat16 [5120, 5120], P(None, 'tp')
- b_q: bfloat16 [5120], P('tp')
- w_k: bfloat16 [5120, 1024], P(None, 'tp')
- b_k: bfloat16 [1024], P('tp')
- w_v: bfloat16 [5120, 1024], P(None, 'tp')
- b_v: bfloat16 [1024], P('tp')
- w_o: bfloat16 [5120, 5120], P('tp')
- g_mlp: bfloat16 [5120], replicated
- w_gate: bfloat16 [5120, 27648], P(None, 'tp')
- w_up: bfloat16 [5120, 27648], P(None, 'tp')
- w_down: bfloat16 [27648, 5120], P('tp')
Outputs:
- output 1: bfloat16 [24, 256, 5120], P('dp', 'tp'), parts along dimension 0
- output 2: bfloat16 [24, 1024, 8, 128], P('dp', None, 'tp'), parts along dimension 0
- output 3: bfloat16 [24, 1024, 8, 128], P('dp', None, 'tp'), parts along dimension 0
There are 2 independent parts. The reference program is written for one: setup_inputs(seed, part) draws one part's arguments, and reference() takes and returns one part's arrays. A program takes and returns all parts, laid end to end along the dimension named above; an argument that names none is the same for every part.
All inputs are finite; a program needn't handle non-finite values.
Results may differ from the reference program's by a relative error of at most 0.0193666.
Values are sent between devices in bfloat16 or wider.
A program may use at most 768 MiB of HBM per device.

```python
import jax
import jax.numpy as jnp
from jax import lax

REQUESTS = 12
CHUNK_LEN = 256
CACHE_SLOTS = 1024
MODEL_DIM = 5120
NUM_HEADS = 40
KV_HEADS = 8
KV_STORE = 8
HEAD_DIM = 128
FFN_DIM = 27648

ROPE_THETA = 1.0e6
NORM_EPS = 1.0e-6
GROUP_SIZE = NUM_HEADS // KV_STORE
KV_REPEAT = KV_STORE // KV_HEADS


def draw_lengths(key):
    keys = jax.random.split(key, 4)
    prefix = jax.random.randint(keys[0], (REQUESTS,), 0, CACHE_SLOTS - CHUNK_LEN + 1)
    valid = jax.random.randint(keys[1], (REQUESTS,), 1, CHUNK_LEN + 1)
    req_ids = jnp.arange(REQUESTS)
    longest = jax.random.randint(keys[2], (), 0, REQUESTS)
    fullest = jax.random.randint(keys[3], (), 0, REQUESTS)
    prefix = jnp.where(req_ids == longest, CACHE_SLOTS - CHUNK_LEN, prefix)
    valid = jnp.where(req_ids == fullest, CHUNK_LEN, valid)
    return prefix.astype(jnp.int32), valid.astype(jnp.int32)


def gauss(key, shape, scale):
    return jax.random.normal(key, shape, jnp.float32) * scale


def kv_copies(values, axis):
    return jnp.repeat(values, KV_REPEAT, axis=axis)


def setup_inputs(seed: int = 0, part: int = 0) -> dict:
    shared = jax.random.split(jax.random.key(seed), 12)
    local = jax.random.split(jax.random.fold_in(jax.random.key(seed + 1), part), 5)
    prefix, valid = draw_lengths(local[0])
    q_cols = NUM_HEADS * HEAD_DIM
    kv_cols = KV_STORE * HEAD_DIM
    hidden = gauss(local[1], (REQUESTS, CHUNK_LEN, MODEL_DIM), 1.0)
    k_cache = kv_copies(gauss(local[2], (REQUESTS, CACHE_SLOTS, KV_HEADS, HEAD_DIM), 1.0), 2)
    v_mean = gauss(local[3], (REQUESTS, 1, KV_HEADS, HEAD_DIM), 1.0)
    v_cache = kv_copies(v_mean + gauss(local[4], (REQUESTS, CACHE_SLOTS, KV_HEADS, HEAD_DIM), 1.5), 2)
    w_k = kv_copies(gauss(shared[3], (MODEL_DIM, KV_HEADS, HEAD_DIM), MODEL_DIM ** -0.5), 1)
    b_k = kv_copies(gauss(shared[4], (KV_HEADS, HEAD_DIM), 1.0), 0)
    w_v = kv_copies(gauss(shared[5], (MODEL_DIM, KV_HEADS, HEAD_DIM), MODEL_DIM ** -0.5), 1)
    b_v = kv_copies(gauss(shared[6], (KV_HEADS, HEAD_DIM), 1.0), 0)
    return {
        "x": hidden.astype(jnp.bfloat16),
        "k_cache": k_cache.astype(jnp.bfloat16),
        "v_cache": v_cache.astype(jnp.bfloat16),
        "prefix_len": prefix,
        "valid_len": valid,
        "g_attn": (1.0 + gauss(shared[0], (MODEL_DIM,), 0.3)).astype(jnp.bfloat16),
        "w_q": gauss(shared[1], (MODEL_DIM, q_cols), 1.5 * MODEL_DIM ** -0.5).astype(jnp.bfloat16),
        "b_q": gauss(shared[2], (q_cols,), 1.0).astype(jnp.bfloat16),
        "w_k": w_k.reshape(MODEL_DIM, kv_cols).astype(jnp.bfloat16),
        "b_k": b_k.reshape(kv_cols).astype(jnp.bfloat16),
        "w_v": w_v.reshape(MODEL_DIM, kv_cols).astype(jnp.bfloat16),
        "b_v": b_v.reshape(kv_cols).astype(jnp.bfloat16),
        "w_o": gauss(shared[7], (q_cols, MODEL_DIM), q_cols ** -0.5).astype(jnp.bfloat16),
        "g_mlp": (1.0 + gauss(shared[8], (MODEL_DIM,), 0.3)).astype(jnp.bfloat16),
        "w_gate": gauss(shared[9], (MODEL_DIM, FFN_DIM), MODEL_DIM ** -0.5).astype(jnp.bfloat16),
        "w_up": gauss(shared[10], (MODEL_DIM, FFN_DIM), MODEL_DIM ** -0.5).astype(jnp.bfloat16),
        "w_down": gauss(shared[11], (FFN_DIM, MODEL_DIM), 1.5 * FFN_DIM ** -0.5).astype(jnp.bfloat16),
    }


def rms_norm(hidden, gain):
    wide_vals = hidden.astype(jnp.float32)
    inv_rms = lax.rsqrt(jnp.mean(wide_vals * wide_vals, axis=-1, keepdims=True) + NORM_EPS)
    return (wide_vals * inv_rms * gain.astype(jnp.float32)).astype(jnp.bfloat16)


def rotate_heads(heads, positions):
    half = heads.shape[-1] // 2
    inv_freq = ROPE_THETA ** (-(jnp.arange(half, dtype=jnp.float32) * 2.0) / heads.shape[-1])
    angles = positions.astype(jnp.float32)[..., None] * inv_freq
    cos_t = jnp.cos(angles)[..., None, :]
    sin_t = jnp.sin(angles)[..., None, :]
    wide = heads.astype(jnp.float32)
    first_half = wide[..., :half]
    second_half = wide[..., half:]
    rotated = jnp.concatenate([first_half * cos_t - second_half * sin_t, second_half * cos_t + first_half * sin_t], axis=-1)
    return rotated.astype(jnp.bfloat16)


def project(hidden, weight, bias):
    total = jnp.dot(hidden, weight, preferred_element_type=jnp.float32)
    return (total + bias.astype(jnp.float32)).astype(jnp.bfloat16)


def reference(x, k_cache, v_cache, prefix_len, valid_len, g_attn, w_q, b_q, w_k, b_k, w_v, b_v, w_o, g_mlp, w_gate, w_up, w_down):
    row_ids = jnp.arange(CHUNK_LEN)
    slot_ids = jnp.arange(CACHE_SLOTS)

    def one_request(req_args):
        hidden, k_rows, v_rows, start, count = req_args
        positions = start + row_ids
        normed = rms_norm(hidden, g_attn)
        queries = rotate_heads(project(normed, w_q, b_q).reshape(CHUNK_LEN, NUM_HEADS, HEAD_DIM), positions)
        keys_new = rotate_heads(project(normed, w_k, b_k).reshape(CHUNK_LEN, KV_STORE, HEAD_DIM), positions)
        values_new = project(normed, w_v, b_v).reshape(CHUNK_LEN, KV_STORE, HEAD_DIM)
        keep = (row_ids < count)[:, None, None]
        k_old = lax.dynamic_slice_in_dim(k_rows, start, CHUNK_LEN, axis=0)
        v_old = lax.dynamic_slice_in_dim(v_rows, start, CHUNK_LEN, axis=0)
        k_rows = lax.dynamic_update_slice_in_dim(k_rows, jnp.where(keep, keys_new, k_old), start, axis=0)
        v_rows = lax.dynamic_update_slice_in_dim(v_rows, jnp.where(keep, values_new, v_old), start, axis=0)
        limit = start + jnp.minimum(row_ids, count - 1)
        visible = slot_ids[None, :] <= limit[:, None]
        query_groups = queries.reshape(CHUNK_LEN, KV_STORE, GROUP_SIZE, HEAD_DIM)

        def one_head(head_args):
            q_head, k_head, v_head = head_args
            scores = jnp.einsum("cgd,sd->gcs", q_head.astype(jnp.float32), k_head.astype(jnp.float32)) * HEAD_DIM ** -0.5
            scores = jnp.where(visible[None], scores, -1.0e30)
            attn_probs = jax.nn.softmax(scores, axis=-1).astype(jnp.bfloat16)
            mixed = jnp.einsum("gcs,sd->cgd", attn_probs.astype(jnp.float32), v_head.astype(jnp.float32))
            return mixed.astype(jnp.bfloat16)

        heads_out = lax.map(one_head, (jnp.moveaxis(query_groups, 1, 0), jnp.moveaxis(k_rows, 1, 0), jnp.moveaxis(v_rows, 1, 0)))
        attended = jnp.moveaxis(heads_out, 0, 1).reshape(CHUNK_LEN, NUM_HEADS * HEAD_DIM)
        attn_out = jnp.dot(attended, w_o, preferred_element_type=jnp.float32).astype(jnp.bfloat16)
        resid_mid = (hidden.astype(jnp.float32) + attn_out.astype(jnp.float32)).astype(jnp.bfloat16)
        normed_mlp = rms_norm(resid_mid, g_mlp)
        gate = jnp.dot(normed_mlp, w_gate, preferred_element_type=jnp.float32)
        up_proj = jnp.dot(normed_mlp, w_up, preferred_element_type=jnp.float32)
        hidden_act = (jax.nn.silu(gate) * up_proj).astype(jnp.bfloat16)
        down = jnp.dot(hidden_act, w_down, preferred_element_type=jnp.float32).astype(jnp.bfloat16)
        result = (resid_mid.astype(jnp.float32) + down.astype(jnp.float32)).astype(jnp.bfloat16)
        return result, k_rows, v_rows

    x_out, k_out, v_out = lax.map(one_request, (x, k_cache, v_cache, prefix_len, valid_len))
    return x_out, k_out, v_out
```

```python
import functools

import jax
import jax.numpy as jnp
from jax import lax
from jax.experimental import pallas as pl
from jax.experimental.pallas import tpu as pltpu
from jax.sharding import PartitionSpec as P

ROPE_THETA = 1.0e6
NORM_EPS = 1.0e-6
BF = jnp.bfloat16
F32 = jnp.float32
R = 2
GU = 128
DN = 256
SUB = 16

AT = dict(
    rs1_relay=0.02,
    rs2_half=0.16,
    ag1_fwd=0.26,
    rs1_fin=0.38,
    rs2_relay=0.52,
    ag1_far=0.64,
    ag2_fwd=0.82,
    rs1_half=0.25,
    ag1_own=0.35,
    ag2_fin=0.95,
)


def rope_tables(prefix, n_tokens, head_dim):
    half = head_dim // 2
    inv_freq = ROPE_THETA ** (-(jnp.arange(half, dtype=F32) * 2.0) / head_dim)
    positions = prefix[:, None] + jnp.arange(n_tokens, dtype=jnp.int32)[None, :]
    angles = positions.astype(F32)[..., None] * inv_freq
    cos_t, sin_t = jnp.cos(angles), jnp.sin(angles)
    return jnp.concatenate([cos_t, cos_t], -1), jnp.concatenate([-sin_t, sin_t], -1)


def layer_kernel(
    p_ref, c_ref, bias_ref, g1_ref, g2_ref, x_hbm, cos_hbm, sin_hbm, kc_hbm, vc_hbm, wq_hbm, wk_hbm, wv_hbm, wo_hbm, wg_hbm, wu_hbm, wd_hbm,
    out_hbm, ko_hbm, vo_hbm, h1_hbm, h2_hbm, sb1_hbm, sb2_hbm, rb1_hbm, rb2_hbm, fb1_hbm, fb2_hbm, x1_hbm,
    w_qkv, w_out, gu_buf, dn_buf, h2v, h1v, act, p1, p2, t_a, t_b, t_c, xin, xmid, xend, hb1, hb2, ob, kcv, vcv, kb, vb, kshift, vshift, cosv, sinv, q_buf, o_buf,
    ag_s, ag_r, rs_s, rs_r, tmp_sem, x_sem, h_sem, st_sem, at_sem, kv_sem, gu_sem, dn_sem, w_sem,
):
    n_chunks, blk, width = x_hbm.shape
    half = blk // R
    tokens, hd = cos_hbm.shape[1], cos_hbm.shape[2]
    slots = kc_hbm.shape[1]
    qn = w_out.shape[0]
    ffn = act.shape[1]
    n_gu, n_dn = ffn // GU, width // DN
    n_dev = h1_hbm.shape[1]
    n_chip = n_dev // 2

    me = lax.axis_index("tp")
    core = lax.rem(me, 2)
    chip = lax.div(me, 2)
    chips = [lax.rem(chip + 2, n_chip), lax.rem(chip + 1, n_chip), lax.rem(chip + 3, n_chip), chip]
    far, right_chip, left_chip, _ = chips
    right, left, sib = 2 * right_chip + core, 2 * left_chip + core, me + 1 - 2 * core

    hbufs, gains = (hb1, hb2), (g1_ref, g2_ref)
    h_all, parts = (h1_hbm, h2_hbm), (p1, p2)
    sbs, rbs, fbs = (sb1_hbm, sb2_hbm), (rb1_hbm, rb2_hbm), (fb1_hbm, fb2_hbm)

    def ag(s, c, k):
        h = h_all[s]
        lo, hi = pl.ds(0, half), pl.ds(half, half)
        lt, rt, ft = 2 * left_chip + core, 2 * right_chip + core, 2 * far + core
        own = hbufs[s]
        src, dst, dev = [
            (own, h.at[c, me], right),
            (own, h.at[c, me], left),
            (own, h.at[c, me], sib),
            (h.at[c, lt, lo], h.at[c, lt, lo], right),
            (h.at[c, rt, hi], h.at[c, rt, hi], left),
            (h.at[c, lt], h.at[c, lt], sib),
            (h.at[c, rt], h.at[c, rt], sib),
            (h.at[c, ft, lo], h.at[c, ft, lo], sib),
            (h.at[c, ft, hi], h.at[c, ft, hi], sib),
        ][k]
        return pltpu.make_async_remote_copy(src, dst, ag_s.at[s, c, k], ag_r.at[s, c, k], device_id={"tp": dev})

    def rs(s, c, k):
        p, lo, hi = parts[s], pl.ds(0, half), pl.ds(half, half)
        if k < 4:
            src, dst, dev = p.at[chips[k], 1 - core], sbs[s].at[c, k], sib
        else:
            src, dst, dev = [
                (p.at[far, core, lo], rbs[s].at[c, 0], right),
                (p.at[far, core, hi], rbs[s].at[c, 1], left),
                (p.at[right_chip, core], fbs[s].at[c, 0], right),
                (p.at[left_chip, core], fbs[s].at[c, 1], left),
            ][k - 4]
        return pltpu.make_async_remote_copy(src, dst, rs_s.at[s, c, k], rs_r.at[s, c, k], device_id={"tp": dev})

    def by_rows(rows, fn):
        def step(i, carry):
            fn(pl.ds(pl.multiple_of(i * SUB, SUB), SUB))
            return carry

        lax.fori_loop(0, rows // SUB, step, 0)

    def f32(v):
        return v.astype(F32)

    def normed(wide, gain):
        inv_rms = lax.rsqrt(jnp.mean(wide * wide, axis=-1, keepdims=True) + NORM_EPS)
        return (wide * inv_rms * f32(gain[...])).astype(BF)

    def own_copy(s, c):
        return pltpu.make_async_copy(hbufs[s], h_all[s].at[c, me], h_sem.at[s])

    def x_copy(c):
        return pltpu.make_async_copy(x_hbm.at[c], xin, x_sem.at[0])

    def ag_send(s, c):
        own_copy(s, c).start()
        for k in range(3):
            ag(s, c, k).start()

    def ag1_own(c):
        x_copy(c).wait()

        def fn(rows):
            hb1[rows, :] = normed(f32(xin[rows, :]), g1_ref)

        by_rows(blk, fn)
        ag_send(0, c)

        @pl.when(c + 1 < n_chunks)
        def _():
            x_copy(c + 1).start()

    def ag_fwd(s, c):
        ag(s, c, 0).wait_recv()
        ag(s, c, 3).start()
        ag(s, c, 1).wait_recv()
        ag(s, c, 4).start()
        ag(s, c, 5).start()
        ag(s, c, 6).start()

    def ag_far(s, c):
        for k in (3, 4):
            ag(s, c, k).wait_recv()
            ag(s, c, k + 4).start()

    def ag_fin(s, c):
        for k in (2, 5, 6, 7, 8):
            ag(s, c, k).wait_recv()
        for k in range(9):
            ag(s, c, k).wait_send()
        own_copy(s, c).wait()

    def rs_pair(s, c):
        for k in range(4):
            rs(s, c, k).start()

    def half_loads(s, c):
        return (pltpu.make_async_copy(sbs[s].at[c, 0], t_a, tmp_sem.at[0]),)

    def rs_half_load(s, c):
        rs(s, c, 0).wait_recv()
        for cp in half_loads(s, c):
            cp.start()

    def rs_half(s, c):
        for cp in half_loads(s, c):
            cp.wait()
        p = parts[s]

        def fn(rows):
            p[far, core, rows, :] = (f32(p[far, core, rows, :]) + f32(t_a[rows, :])).astype(BF)

        by_rows(blk, fn)
        rs(s, c, 4).start()
        rs(s, c, 5).start()

    def relay_loads(s, c):
        return (
            pltpu.make_async_copy(sbs[s].at[c, 1], t_a, tmp_sem.at[0]),
            pltpu.make_async_copy(sbs[s].at[c, 2], t_b, tmp_sem.at[1]),
            pltpu.make_async_copy(rbs[s].at[c, 0], t_c.at[pl.ds(0, half)], tmp_sem.at[2]),
            pltpu.make_async_copy(rbs[s].at[c, 1], t_c.at[pl.ds(half, half)], tmp_sem.at[3]),
        )

    def rs_relay_load(s, c):
        loads = relay_loads(s, c)
        for k, cp in zip((1, 2, 4, 5), loads):
            rs(s, c, k).wait_recv()
            cp.start()

    def rs_relay(s, c):
        for cp in relay_loads(s, c):
            cp.wait()
        p = parts[s]

        def first(i):
            lo = pl.ds(pl.multiple_of(i * SUB, SUB), SUB)
            hi = pl.ds(pl.multiple_of(half + i * SUB, SUB), SUB)
            p[right_chip, core, lo, :] = (f32(p[right_chip, core, lo, :]) + f32(t_a[lo, :]) + f32(t_c[lo, :])).astype(BF)
            p[right_chip, core, hi, :] = (f32(p[right_chip, core, hi, :]) + f32(t_a[hi, :])).astype(BF)
            p[left_chip, core, lo, :] = (f32(p[left_chip, core, lo, :]) + f32(t_b[lo, :])).astype(BF)
            p[left_chip, core, hi, :] = (f32(p[left_chip, core, hi, :]) + f32(t_b[hi, :]) + f32(t_c[hi, :])).astype(BF)

        def step(i, carry):
            first(i)
            return carry

        lax.fori_loop(0, half // SUB, step, 0)
        rs(s, c, 6).start()
        rs(s, c, 7).start()

    def fin_loads(s, c):
        return (
            pltpu.make_async_copy(sbs[s].at[c, 3], t_a, tmp_sem.at[0]),
            pltpu.make_async_copy(fbs[s].at[c, 0], t_b, tmp_sem.at[1]),
            pltpu.make_async_copy(fbs[s].at[c, 1], t_c, tmp_sem.at[2]),
        )

    def rs_fin_load(s, c):
        for k, cp in zip((3, 6, 7), fin_loads(s, c)):
            rs(s, c, k).wait_recv()
            cp.start()

    def rs_total(s, rows):
        p = parts[s]
        return (f32(p[chip, core, rows, :]) + f32(t_a[rows, :]) + f32(t_b[rows, :]) + f32(t_c[rows, :])).astype(BF)

    def rs_sent(s, c):
        for k in range(8):
            rs(s, c, k).wait_send()

    def xmid_copy(c):
        return pltpu.make_async_copy(x_hbm.at[c], xmid, x_sem.at[1])

    def x1_store(c):
        return pltpu.make_async_copy(xmid, x1_hbm.at[c], st_sem.at[0])

    def xend_copy(c):
        return pltpu.make_async_copy(x1_hbm.at[c], xend, x_sem.at[2])

    def out_store(c):
        return pltpu.make_async_copy(ob, out_hbm.at[c], st_sem.at[1])

    def rs1_fin(c):
        for cp in fin_loads(0, c):
            cp.wait()
        xmid_copy(c).wait()

        def fn(rows):
            mid = (f32(xmid[rows, :]) + f32(rs_total(0, rows))).astype(BF)
            xmid[rows, :] = mid
            hb2[rows, :] = normed(f32(mid), g2_ref)

        by_rows(blk, fn)
        x1_store(c).start()
        ag_send(1, c)

    def rs2_fin(c):
        rs_fin_load(1, c)
        for cp in fin_loads(1, c):
            cp.wait()
        xend_copy(c).wait()

        def fn(rows):
            ob[rows, :] = (f32(xend[rows, :]) + f32(rs_total(1, rows))).astype(BF)

        by_rows(blk, fn)
        out_store(c).start()
        rs_sent(1, c)

    def att_loads(a, r):
        req = a * R + r
        return (
            pltpu.make_async_copy(h1_hbm.at[a, :, pl.ds(pl.multiple_of(r * half, half), half)], h1v, at_sem.at[0]),
            pltpu.make_async_copy(kc_hbm.at[req], kcv, at_sem.at[1]),
            pltpu.make_async_copy(vc_hbm.at[req], vcv, at_sem.at[2]),
            pltpu.make_async_copy(cos_hbm.at[req], cosv, at_sem.at[3]),
            pltpu.make_async_copy(sin_hbm.at[req], sinv, at_sem.at[4]),
        )

    def attend(a, r):
        req = a * R + r
        for cp in att_loads(a, r):
            cp.wait()
        p, c = p_ref[req], c_ref[req]
        qkv = jnp.dot(h1v[...].reshape(tokens, width), w_qkv[...], preferred_element_type=F32) + f32(bias_ref[...])
        qkv = f32(qkv.astype(BF))
        cos, sin = cosv[...], sinv[...]

        def rope(v):
            return v * cos + pltpu.roll(v, hd // 2, 1) * sin

        for j in range(qn // hd):
            q_buf[:, j * hd : (j + 1) * hd] = rope(qkv[:, j * hd : (j + 1) * hd]).astype(BF)
        kshift[slots : slots + tokens, :] = rope(qkv[:, qn : qn + hd])
        vshift[slots : slots + tokens, :] = qkv[:, qn + hd :]
        slot = lax.broadcasted_iota(jnp.int32, (slots, hd), 0)
        new = (slot >= p) & (slot < p + c)
        kb[...] = jnp.where(new, kshift[pl.ds(slots - p, slots), :], f32(kcv[...])).astype(BF)
        vb[...] = jnp.where(new, vshift[pl.ds(slots - p, slots), :], f32(vcv[...])).astype(BF)
        stores = (pltpu.make_async_copy(kb, ko_hbm.at[req], kv_sem.at[0]), pltpu.make_async_copy(vb, vo_hbm.at[req], kv_sem.at[1]))
        for cp in stores:
            cp.start()

        @pl.when(r + 1 < R)
        def _():
            for cp in att_loads(a, r + 1):
                cp.start()

        limit = p + jnp.minimum(lax.broadcasted_iota(jnp.int32, (tokens, slots), 0), c - 1)
        visible = lax.broadcasted_iota(jnp.int32, (tokens, slots), 1) <= limit
        for j in range(qn // hd):
            cols = slice(j * hd, (j + 1) * hd)
            scores = lax.dot_general(q_buf[:, cols], kb[...], (((1,), (1,)), ((), ())), preferred_element_type=F32) * (hd**-0.5)
            scores = jnp.where(visible, scores, -1.0e30)
            expd = jnp.exp(scores - jnp.max(scores, axis=1, keepdims=True))
            probs = (expd * (1.0 / jnp.sum(expd, axis=1, keepdims=True))).astype(BF)
            o_buf[:, cols] = jnp.dot(probs, vb[...], preferred_element_type=F32).astype(BF)

        def out_tile(i, carry):
            cols = pl.ds(pl.multiple_of(i * 2 * DN, 2 * DN), 2 * DN)
            tile = jnp.dot(o_buf[...], w_out[:, cols], preferred_element_type=F32).astype(BF)
            p1[:, :, pl.ds(pl.multiple_of(r * half, half), half), cols] = tile.reshape(n_chip, 2, half, 2 * DN)
            return carry

        lax.fori_loop(0, width // (2 * DN), out_tile, 0)
        for cp in stores:
            cp.wait()

    def gu_copies(tile, slot):
        cols = pl.ds(pl.multiple_of(tile * GU, GU), GU)
        return (
            pltpu.make_async_copy(wg_hbm.at[:, cols], gu_buf.at[slot, :, pl.ds(0, GU)], gu_sem.at[slot, 0]),
            pltpu.make_async_copy(wu_hbm.at[:, cols], gu_buf.at[slot, :, pl.ds(GU, GU)], gu_sem.at[slot, 1]),
        )

    def dn_copy(tile, slot):
        cols = pl.ds(pl.multiple_of(tile * DN, DN), DN)
        return pltpu.make_async_copy(wd_hbm.at[:, cols], dn_buf.at[slot], dn_sem.at[slot])

    def h2_load(c):
        return pltpu.make_async_copy(h2_hbm.at[c], h2v, h_sem.at[2])

    def qkv_loads():
        return (
            pltpu.make_async_copy(wq_hbm, w_qkv.at[:, pl.ds(0, qn)], w_sem.at[0]),
            pltpu.make_async_copy(wk_hbm, w_qkv.at[:, pl.ds(qn, hd)], w_sem.at[1]),
            pltpu.make_async_copy(wv_hbm, w_qkv.at[:, pl.ds(qn + hd, hd)], w_sem.at[2]),
            pltpu.make_async_copy(wo_hbm, w_out, w_sem.at[3]),
        )

    x_copy(0).start()
    barrier = pltpu.get_barrier_semaphore()
    for dev in (right, left, sib):
        pl.semaphore_signal(barrier, inc=1, device_id={"tp": dev})
    pl.semaphore_wait(barrier, 3)
    ag1_own(0)
    for cp in qkv_loads():
        cp.start()
    for cp in gu_copies(0, 0):
        cp.start()
    kshift[...] = jnp.zeros_like(kshift)
    vshift[...] = jnp.zeros_like(vshift)
    for cp in qkv_loads():
        cp.wait()

    def ok(c):
        return (c >= 0) & (c < n_chunks)

    def step(t, carry):
        mlp, mid, old = t - 2, t - 1, t - 3

        def event(now, name, phase, chunk, fn, late=0):
            at = min(int(AT[name] * phase) + late, phase - 1)

            @pl.when((now == at) & ok(chunk))
            def _():
                fn(chunk)

        def relay1_load(c):
            xmid_copy(c).start()
            rs_relay_load(0, c)

        def relay2_load(c):
            xend_copy(c).start()
            rs_relay_load(1, c)

        def gu_step(j, carry):
            event(j, "rs1_relay", n_gu, mid, relay1_load)
            event(j, "rs1_relay", n_gu, mid, lambda c: rs_relay(0, c), 1)
            event(j, "rs2_half", n_gu, old, lambda c: rs_half_load(1, c))
            event(j, "rs2_half", n_gu, old, lambda c: rs_half(1, c), 1)
            event(j, "ag1_fwd", n_gu, t, lambda c: ag_fwd(0, c))
            event(j, "rs1_fin", n_gu, mid, lambda c: rs_fin_load(0, c))
            event(j, "rs1_fin", n_gu, mid, rs1_fin, 1)
            event(j, "rs2_relay", n_gu, old, relay2_load)
            event(j, "rs2_relay", n_gu, old, lambda c: rs_relay(1, c), 1)
            event(j, "ag1_far", n_gu, t, lambda c: ag_far(0, c))
            event(j, "ag2_fwd", n_gu, mid, lambda c: ag_fwd(1, c))

            @pl.when(ok(mlp))
            def _():
                slot = lax.rem(j, 2)

                @pl.when(j == 0)
                def _():
                    dn_copy(0, 0).start()
                    h2_load(mlp).wait()

                @pl.when(j + 1 < n_gu)
                def _():
                    for cp in gu_copies(j + 1, 1 - slot):
                        cp.start()

                for cp in gu_copies(j, slot):
                    cp.wait()
                both = jnp.dot(h2v[...].reshape(n_dev * blk, width), gu_buf[slot], preferred_element_type=F32)
                gate, up = both[:, :GU], both[:, GU:]
                act[:, pl.ds(pl.multiple_of(j * GU, GU), GU)] = (jax.nn.silu(gate) * up).astype(BF)

            return carry

        lax.fori_loop(0, n_gu, gu_step, 0)

        @pl.when(ok(mlp) & (mlp + 1 < n_chunks))
        def _():
            for cp in gu_copies(0, 0):
                cp.start()

        @pl.when(ok(mid))
        def _():
            rs_sent(0, mid)
            x1_store(mid).wait()

        @pl.when(ok(t))
        def _():
            ag_fin(0, t)
            for cp in att_loads(t, 0):
                cp.start()

        @pl.when(ok(old))
        def _():
            rs2_fin(old)

        def att_step(r, carry):
            @pl.when(ok(t))
            def _():
                attend(t, r)

            @pl.when((r == 0) & ok(mid))
            def _():
                ag_far(1, mid)

            return carry

        lax.fori_loop(0, R, att_step, 0)

        @pl.when(ok(t))
        def _():
            rs_pair(0, t)

        def dn_step(j, carry):
            event(j, "rs1_half", n_dn, t, lambda c: rs_half_load(0, c))
            event(j, "rs1_half", n_dn, t, lambda c: rs_half(0, c), 1)
            event(j, "ag1_own", n_dn, t + 1, ag1_own)

            def fin2(c):
                ag_fin(1, c)
                h2_load(c).start()

            event(j, "ag2_fin", n_dn, mid, fin2)

            @pl.when(ok(mlp))
            def _():
                slot = lax.rem(j, 2)

                @pl.when(j + 1 < n_dn)
                def _():
                    dn_copy(j + 1, 1 - slot).start()

                dn_copy(j, slot).wait()
                tile = jnp.dot(act[...], dn_buf[slot], preferred_element_type=F32).astype(BF)
                p2[:, :, :, pl.ds(pl.multiple_of(j * DN, DN), DN)] = tile.reshape(n_chip, 2, blk, DN)

            return carry

        lax.fori_loop(0, n_dn, dn_step, 0)

        @pl.when(ok(old))
        def _():
            out_store(old).wait()

        @pl.when(ok(mlp))
        def _():
            rs_pair(1, mlp)

        return carry

    lax.fori_loop(0, n_chunks + 3, step, 0)


def fused_layer(x, cos, sin, bias, k_cache, v_cache, prefix, valid, g_attn, g_mlp, w_q, w_k, w_v, w_o, w_gate, w_up, w_down, n_dev):
    n_req, rows, width = x.shape
    n_chunks, blk = n_req // R, R * rows
    slots, hd = k_cache.shape[1:]
    tokens, qn, ffn = n_dev * rows, w_q.shape[1], w_gate.shape[1]
    n_chip = n_dev // 2
    hbm, smem, vmem = (pl.BlockSpec(memory_space=m) for m in (pl.ANY, pltpu.SMEM, pltpu.VMEM))
    chunked = lambda *s: jax.ShapeDtypeStruct((n_chunks, *s, width), BF)
    out_shape = [
        chunked(blk),
        jax.ShapeDtypeStruct(k_cache.shape, BF),
        jax.ShapeDtypeStruct(v_cache.shape, BF),
        chunked(n_dev, blk),
        chunked(n_dev, blk),
        chunked(n_chip, blk),
        chunked(n_chip, blk),
        chunked(2, rows),
        chunked(2, rows),
        chunked(2, blk),
        chunked(2, blk),
        chunked(blk),
    ]
    dma = lambda *s: pltpu.SemaphoreType.DMA(s)
    rows_buf = pltpu.VMEM((blk, width), BF)
    scratch = [
        pltpu.VMEM((width, qn + 2 * hd), BF),
        pltpu.VMEM((qn, width), BF),
        pltpu.VMEM((2, width, 2 * GU), BF),
        pltpu.VMEM((2, ffn, DN), BF),
        pltpu.VMEM((n_dev, blk, width), BF),
        pltpu.VMEM((n_dev, rows, width), BF),
        pltpu.VMEM((n_dev * blk, ffn), BF),
        pltpu.VMEM((n_chip, 2, blk, width), BF),
        pltpu.VMEM((n_chip, 2, blk, width), BF),
        *[rows_buf] * 9,
        *[pltpu.VMEM((slots, hd), BF)] * 4,
        *[pltpu.VMEM((2 * slots, hd), F32)] * 2,
        *[pltpu.VMEM((tokens, hd), F32)] * 2,
        *[pltpu.VMEM((tokens, qn), BF)] * 2,
        dma(2, n_chunks, 9),
        dma(2, n_chunks, 9),
        dma(2, n_chunks, 8),
        dma(2, n_chunks, 8),
        dma(4),
        dma(3),
        dma(3),
        dma(2),
        dma(5),
        dma(2),
        dma(2, 2),
        dma(2),
        dma(4),
    ]
    res = pl.pallas_call(
        layer_kernel,
        in_specs=[smem, smem, vmem, vmem, vmem] + [hbm] * 12,
        out_specs=[hbm] * len(out_shape),
        out_shape=out_shape,
        scratch_shapes=scratch,
        compiler_params=pltpu.CompilerParams(vmem_limit_bytes=67_000_000, collective_id=0, has_side_effects=True),
        name="layer",
    )(prefix, valid, bias, g_attn[None], g_mlp[None], x.reshape(n_chunks, blk, width), cos, sin, k_cache, v_cache, w_q, w_k, w_v, w_o, w_gate, w_up, w_down)
    return res[0].reshape(x.shape), res[1], res[2]


def solution(mesh):
    row_spec = P("dp", "tp", None)
    cache_spec = P("dp", None, "tp", None)
    req_spec = P("dp")
    rep_spec = P(None)
    col_spec = P(None, "tp")
    bias_spec = P("tp")
    down_spec = P("tp", None)
    n_dev = mesh.shape["tp"]

    def layer(x_rows, k_cache, v_cache, prefix, valid, g_attn, w_q, b_q, w_k, b_k, w_v, b_v, w_o, g_mlp, w_gate, w_up, w_down):
        n_req, rows, _ = x_rows.shape
        slots, hd = k_cache.shape[1], k_cache.shape[3]
        keys, vals = k_cache.reshape(n_req, slots, hd), v_cache.reshape(n_req, slots, hd)
        cos, sin = rope_tables(prefix, rows * n_dev, hd)
        bias = jnp.concatenate([b_q, b_k, b_v])[None]
        out, k_out, v_out = fused_layer(x_rows, cos, sin, bias, keys, vals, prefix, valid, g_attn, g_mlp, w_q, w_k, w_v, w_o, w_gate, w_up, w_down, n_dev)
        return out, k_out.reshape(k_cache.shape), v_out.reshape(v_cache.shape)

    in_specs = (row_spec, cache_spec, cache_spec, req_spec, req_spec, rep_spec, col_spec, bias_spec, col_spec, bias_spec, col_spec, bias_spec, down_spec, rep_spec, col_spec, col_spec, down_spec)
    return jax.shard_map(layer, mesh=mesh, in_specs=in_specs, out_specs=(row_spec, cache_spec, cache_spec), check_vma=False)
```

```python
import jax
import jax.numpy as jnp
import numpy as np
from jax import lax
from jax.experimental import pallas as pl
from jax.experimental.pallas import tpu as pltpu
from jax.sharding import PartitionSpec as P

ROPE_THETA = 1.0e6
NORM_EPS = 1.0e-6
LOG2_E = 1.4426950408889634
BF = jnp.bfloat16
F32 = jnp.float32
R = 2
GU = 384
DN = 512
GU_SLOTS, DN_SLOTS = 2, 2
QA = 512
SUB = 16
LEAD = 3

GU_PARTS, DN_PARTS = 9, 5


def layer_kernel(
    p_ref, c_ref, bias_ref, g1_ref, g2_ref, freq_ref, x_hbm, kc_hbm, vc_hbm, wq_hbm, wk_hbm, wv_hbm, wo_hbm, wg_hbm, wu_hbm, wd_hbm,
    out_hbm, ko_hbm, vo_hbm, h1_hbm, h2_hbm, sb1_hbm, sb2_hbm, rb1_hbm, rb2_hbm, fb1_hbm, fb2_hbm, x1_hbm, cs_hbm,
    w_out, gu_buf, dn_buf, h2v, h1v, act, pp, t_a, t_b, t_c, xin, xmid, xend, hb1, hb2, kb, vb, shift, csv, sbuf,
    ag_s, ag_r, rs_s, rs_r, tmp_sem, x_sem, h_sem, st_sem, at_sem, kv_sem, gu_sem, dn_sem, w_sem, h2_sem,
):
    n_chunks, blk, width = x_hbm.shape
    half = blk // R
    tokens, hd = cs_hbm.shape[1], cs_hbm.shape[2]
    slots = kc_hbm.shape[1]
    qn = w_out.shape[0]
    ffn = act.shape[1]
    n_gu, n_dn = ffn // GU, width // DN
    n_dev = h1_hbm.shape[1]
    n_chip = n_dev // 2

    me = lax.axis_index("tp")
    core = lax.rem(me, 2)
    chip = lax.div(me, 2)
    chips = [lax.rem(chip + 2, n_chip), lax.rem(chip + 1, n_chip), lax.rem(chip + 3, n_chip), chip]
    far, right_chip, left_chip, _ = chips
    right, left, sib = 2 * right_chip + core, 2 * left_chip + core, me + 1 - 2 * core

    hbufs, gains = (hb1, hb2), (g1_ref, g2_ref)
    h_all = (h1_hbm, h2_hbm)
    sbs, rbs, fbs = (sb1_hbm, sb2_hbm), (rb1_hbm, rb2_hbm), (fb1_hbm, fb2_hbm)

    def part(s, c):
        return pp.at[1 if s else jnp.where(c == 1, 1, 0)]

    def h_slot(s, c):
        return 0 if s else lax.rem(c, 2)

    def ag(s, c, k):
        h = h_all[s]
        lo, hi = pl.ds(0, half), pl.ds(half, half)
        lt, rt, ft = 2 * left_chip + core, 2 * right_chip + core, 2 * far + core
        own = hbufs[s].at[h_slot(s, c)]
        src, dst, dev = [
            (own, h.at[c, me], right),
            (own, h.at[c, me], left),
            (own, h.at[c, me], sib),
            (h.at[c, lt, lo], h.at[c, lt, lo], right),
            (h.at[c, rt, hi], h.at[c, rt, hi], left),
            (h.at[c, lt], h.at[c, lt], sib),
            (h.at[c, rt], h.at[c, rt], sib),
            (h.at[c, ft, lo], h.at[c, ft, lo], sib),
            (h.at[c, ft, hi], h.at[c, ft, hi], sib),
        ][k]
        return pltpu.make_async_remote_copy(src, dst, ag_s.at[s, c, k], ag_r.at[s, c, k], device_id={"tp": dev})

    def rs(s, c, k, cut=None):
        col, row = (pl.ds(0, width), c) if cut is None else (pl.ds(*cut[:2]), n_chunks - 1 + cut[2])
        p, lo, hi = part(s, c), pl.ds(0, half), pl.ds(half, half)
        all_rows = pl.ds(0, blk)
        if k < 4:
            src, dst, dev = p.at[chips[k], 1 - core, all_rows, col], sbs[s].at[c, k, all_rows, col], sib
        else:
            src, dst, dev = [
                (p.at[far, core, lo, col], rbs[s].at[c, 0, pl.ds(0, half), col], right),
                (p.at[far, core, hi, col], rbs[s].at[c, 1, pl.ds(0, half), col], left),
                (p.at[right_chip, core, all_rows, col], fbs[s].at[c, 0, all_rows, col], right),
                (p.at[left_chip, core, all_rows, col], fbs[s].at[c, 1, all_rows, col], left),
            ][k - 4]
        return pltpu.make_async_remote_copy(src, dst, rs_s.at[s, row, k], rs_r.at[s, row, k], device_id={"tp": dev})

    def by_rows(rows, fn):
        def step(i, carry):
            fn(pl.ds(pl.multiple_of(i * SUB, SUB), SUB))
            return carry

        lax.fori_loop(0, rows // SUB, step, 0)

    def f32(v):
        return v.astype(F32)

    def normed(wide, gain):
        inv_rms = lax.rsqrt(jnp.mean(wide * wide, axis=-1, keepdims=True) + NORM_EPS)
        return (wide * inv_rms * f32(gain[...])).astype(BF)

    def own_copy(s, c):
        slot = h_slot(s, c)
        return pltpu.make_async_copy(hbufs[s].at[slot], h_all[s].at[c, me], h_sem.at[s, slot])

    def x_copy(c):
        return pltpu.make_async_copy(x_hbm.at[c], xin, x_sem.at[0])

    def ag_send(s, c):
        own_copy(s, c).start()
        for k in range(3):
            ag(s, c, k).start()

    def ag1_own(c):
        x_copy(c).wait()

        def fn(rows):
            hb1[h_slot(0, c), rows, :] = normed(f32(xin[rows, :]), g1_ref)

        by_rows(blk, fn)
        ag_send(0, c)

        @pl.when(c + 1 < n_chunks)
        def _():
            x_copy(c + 1).start()

    def ag_fwd(s, c):
        ag(s, c, 0).wait_recv()
        ag(s, c, 3).start()
        ag(s, c, 1).wait_recv()
        ag(s, c, 4).start()
        ag(s, c, 5).start()
        ag(s, c, 6).start()

    def ag_far(s, c):
        for k in (3, 4):
            ag(s, c, k).wait_recv()
            ag(s, c, k + 4).start()

    def ag_fin(s, c):
        for k in (2, 5, 6, 7, 8):
            ag(s, c, k).wait_recv()
        for k in range(9):
            ag(s, c, k).wait_send()
        own_copy(s, c).wait()

    def rs_pair(s, c, cut=None):
        for k in range(4):
            rs(s, c, k, cut).start()

    def loads(srcs, cut):
        col = pl.ds(0, width) if cut is None else pl.ds(*cut[:2])
        return [
            pltpu.make_async_copy(src.at[:, col], dst.at[:, col], tmp_sem.at[i]) for i, (src, dst) in enumerate(srcs)
        ]

    def half_loads(s, c, cut):
        return loads([(sbs[s].at[c, 0], t_a)], cut)

    def rs_half_load(s, c, cut=None):
        rs(s, c, 0, cut).wait_recv()
        for cp in half_loads(s, c, cut):
            cp.start()

    def rs_half(s, c, cut=None):
        for cp in half_loads(s, c, cut):
            cp.wait()
        p, col = part(s, c), slice(None) if cut is None else pl.ds(*cut[:2])

        def fn(rows):
            p[far, core, rows, col] = (f32(p[far, core, rows, col]) + f32(t_a[rows, col])).astype(BF)

        by_rows(blk, fn)
        rs(s, c, 4, cut).start()
        rs(s, c, 5, cut).start()

    def relay_loads(s, c, cut):
        lo, hi = t_c.at[pl.ds(0, half)], t_c.at[pl.ds(half, half)]
        return loads([(sbs[s].at[c, 1], t_a), (sbs[s].at[c, 2], t_b), (rbs[s].at[c, 0], lo), (rbs[s].at[c, 1], hi)], cut)

    def rs_relay_load(s, c, cut=None):
        for k, cp in zip((1, 2, 4, 5), relay_loads(s, c, cut)):
            rs(s, c, k, cut).wait_recv()
            cp.start()

    def rs_relay(s, c, cut=None):
        for cp in relay_loads(s, c, cut):
            cp.wait()
        p, col = part(s, c), slice(None) if cut is None else pl.ds(*cut[:2])

        def step(i, carry):
            lo = pl.ds(pl.multiple_of(i * SUB, SUB), SUB)
            hi = pl.ds(pl.multiple_of(half + i * SUB, SUB), SUB)
            p[right_chip, core, lo, col] = (f32(p[right_chip, core, lo, col]) + f32(t_a[lo, col]) + f32(t_c[lo, col])).astype(BF)
            p[right_chip, core, hi, col] = (f32(p[right_chip, core, hi, col]) + f32(t_a[hi, col])).astype(BF)
            p[left_chip, core, lo, col] = (f32(p[left_chip, core, lo, col]) + f32(t_b[lo, col])).astype(BF)
            p[left_chip, core, hi, col] = (f32(p[left_chip, core, hi, col]) + f32(t_b[hi, col]) + f32(t_c[hi, col])).astype(BF)
            return carry

        lax.fori_loop(0, half // SUB, step, 0)
        rs(s, c, 6, cut).start()
        rs(s, c, 7, cut).start()

    def fin_loads(s, c, cut):
        return loads([(sbs[s].at[c, 3], t_a), (fbs[s].at[c, 0], t_b), (fbs[s].at[c, 1], t_c)], cut)

    def rs_fin_load(s, c, cut=None):
        for k, cp in zip((3, 6, 7), fin_loads(s, c, cut)):
            rs(s, c, k, cut).wait_recv()
            cp.start()

    def rs_total(s, c, rows, col=slice(None)):
        p = part(s, c)
        return (f32(p[chip, core, rows, col]) + f32(t_a[rows, col]) + f32(t_b[rows, col]) + f32(t_c[rows, col])).astype(BF)

    def rs_sent(s, c, cut=None):
        for k in range(8):
            rs(s, c, k, cut).wait_send()

    def xmid_copy(c):
        return pltpu.make_async_copy(x_hbm.at[c], xmid, x_sem.at[1])

    def x1_store(c):
        return pltpu.make_async_copy(xmid, x1_hbm.at[c], st_sem.at[0])

    def xend_copy(c):
        return pltpu.make_async_copy(x1_hbm.at[c], xend, x_sem.at[2])

    def out_store(c):
        return pltpu.make_async_copy(xend, out_hbm.at[c], st_sem.at[1])

    def rs1_fin_load(c):
        @pl.when(c > 0)
        def _():
            x1_store(c - 1).wait()

        xmid_copy(c).start()
        rs_fin_load(0, c)

    def rs1_fin(c):
        for cp in fin_loads(0, c, None):
            cp.wait()
        xmid_copy(c).wait()

        def fn(rows):
            mid = (f32(xmid[rows, :]) + f32(rs_total(0, c, rows))).astype(BF)
            xmid[rows, :] = mid
            hb2[0, rows, :] = normed(f32(mid), g2_ref)

        by_rows(blk, fn)
        x1_store(c).start()
        ag_send(1, c)

    def rs2_fin_load(c):
        @pl.when(c > 0)
        def _():
            out_store(c - 1).wait()

        xend_copy(c).start()
        rs_fin_load(1, c)

    def rs2_add(c, cut=None):
        for cp in fin_loads(1, c, cut):
            cp.wait()
        col = slice(None) if cut is None else pl.ds(*cut[:2])

        def fn(rows):
            xend[rows, col] = (f32(xend[rows, col]) + f32(rs_total(1, c, rows, col))).astype(BF)

        by_rows(blk, fn)

    def rs2_fin(c):
        xend_copy(c).wait()
        rs2_add(c)
        out_store(c).start()
        rs_sent(1, c)

    def att_loads(a, r):
        return (
            pltpu.make_async_copy(h1_hbm.at[a, :, pl.ds(pl.multiple_of(r * half, half), half)], h1v, at_sem.at[0]),
            pltpu.make_async_copy(cs_hbm.at[a * R + r], csv, at_sem.at[3]),
        )

    def cache_loads(a, r):
        return (
            pltpu.make_async_copy(kc_hbm.at[a * R + r], kb, at_sem.at[1]),
            pltpu.make_async_copy(vc_hbm.at[a * R + r], vb, at_sem.at[2]),
        )

    def table(req, carry):
        pos = p_ref[req] + lax.broadcasted_iota(jnp.int32, (tokens, hd), 0)
        angles = f32(pos) * freq_ref[...]
        first = lax.broadcasted_iota(jnp.int32, (tokens, hd), 1) < hd // 2
        csv[...] = jnp.where(first, jnp.cos(angles), jnp.sin(angles))
        cp = pltpu.make_async_copy(csv, cs_hbm.at[req], at_sem.at[3])
        cp.start()
        cp.wait()
        return carry

    def attend(a, r):
        req = a * R + r
        p_out = part(0, a)
        for cp in (*att_loads(a, r), *cache_loads(a, r)):
            cp.wait()
        fresh = (r == 0) & ((a == 0) | (a >= LEAD))
        h = h1v[...].reshape(tokens, width)

        def project(cps, slot, lo, size):
            @pl.when(fresh)
            def _():
                for cp in cps:
                    cp.wait()

            total = jnp.dot(h, gu_buf[slot, :, 0:size], preferred_element_type=F32)
            return f32((total + f32(bias_ref[:, lo : lo + size])).astype(BF))

        some_q = project(qa_loads(), 1, 0, QA)
        rest = project(qb_loads(), 0, QA, qn + 2 * hd - QA)
        p, c = p_ref[req], c_ref[req]
        cs = csv[...]
        sc = pltpu.roll(cs, hd // 2, 1)
        first = lax.broadcasted_iota(jnp.int32, (tokens, hd), 1) < hd // 2
        cos, sin = jnp.where(first, cs, sc), jnp.where(first, -sc, cs)

        def head(j):
            return some_q[:, j * hd : (j + 1) * hd] if j * hd < QA else rest[:, j * hd - QA : (j + 1) * hd - QA]

        def rope(v):
            return v * cos + pltpu.roll(v, hd // 2, 1) * sin

        n_heads, groups = qn // hd, tokens // blk
        for j in range(n_heads):
            h2v[0:groups, :, j * hd : (j + 1) * hd] = rope(head(j)).astype(BF).reshape(groups, blk, hd)
        slot = lax.broadcasted_iota(jnp.int32, (slots, hd), 0)
        new = (slot >= p) & (slot < p + c)
        shift[slots : slots + tokens, :] = rope(head(n_heads))
        kb[...] = jnp.where(new, shift[pl.ds(slots - p, slots), :], f32(kb[...])).astype(BF)
        shift[slots : slots + tokens, :] = head(n_heads + 1)
        vb[...] = jnp.where(new, shift[pl.ds(slots - p, slots), :], f32(vb[...])).astype(BF)
        stores = (pltpu.make_async_copy(kb, ko_hbm.at[req], kv_sem.at[0]), pltpu.make_async_copy(vb, vo_hbm.at[req], kv_sem.at[1]))
        for cp in stores:
            cp.start()

        @pl.when(r + 1 < R)
        def _():
            for cp in att_loads(a, r + 1):
                cp.start()

        @pl.when((r == R - 1) & (a >= LEAD - 1))
        def _():
            start_gu()

        def scores(j):
            q = h2v[0:groups, :, j * hd : (j + 1) * hd].reshape(tokens, hd)
            return lax.dot_general(q, kb[...], (((1,), (1,)), ((), ())), preferred_element_type=F32)

        limit = p + jnp.minimum(lax.broadcasted_iota(jnp.int32, (tokens, slots), 0), c - 1)
        visible = lax.broadcasted_iota(jnp.int32, (tokens, slots), 1) <= limit
        sbuf[0] = scores(0)
        for j in range(n_heads):
            if j + 1 < n_heads:
                sbuf[(j + 1) % 2] = scores(j + 1)
            masked = jnp.where(visible, sbuf[j % 2], -1.0e30)
            expd = jnp.exp2((masked - jnp.max(masked, axis=1, keepdims=True)) * (hd**-0.5 * LOG2_E))
            probs = (expd * (1.0 / jnp.sum(expd, axis=1, keepdims=True))).astype(BF)
            mixed = jnp.dot(probs, vb[...], preferred_element_type=F32).astype(BF)
            h2v[groups : 2 * groups, :, j * hd : (j + 1) * hd] = mixed.reshape(groups, blk, hd)
        for cp in stores:
            cp.wait()

        @pl.when(r + 1 < R)
        def _():
            for cp in cache_loads(a, r + 1):
                cp.start()

        heads = h2v[groups : 2 * groups, :, 0:qn].reshape(tokens, qn)
        out = jnp.dot(heads, w_out[...], preferred_element_type=F32).astype(BF)
        p_out[:, :, pl.ds(pl.multiple_of(r * half, half), half), :] = out.reshape(n_chip, 2, half, width)

    def gu_copies(tile, slot):
        cols = pl.ds(pl.multiple_of(tile * GU, GU), GU)
        return (
            pltpu.make_async_copy(wg_hbm.at[:, cols], gu_buf.at[slot, :, pl.ds(0, GU)], gu_sem.at[slot, 0]),
            pltpu.make_async_copy(wu_hbm.at[:, cols], gu_buf.at[slot, :, pl.ds(GU, GU)], gu_sem.at[slot, 1]),
        )

    def dn_copy(tile, slot):
        cols = pl.ds(pl.multiple_of(tile * DN, DN), DN)
        return pltpu.make_async_copy(wd_hbm.at[:, cols], dn_buf.at[slot], dn_sem.at[slot])

    def h2_load(c):
        return pltpu.make_async_copy(h2_hbm.at[c], h2v, h2_sem)

    def start_gu():
        for tile in range(GU_SLOTS - 1):
            for cp in gu_copies(tile, tile):
                cp.start()

    def qa_loads():
        return (pltpu.make_async_copy(wq_hbm.at[:, pl.ds(0, QA)], gu_buf.at[1, :, pl.ds(0, QA)], w_sem.at[0]),)

    def qb_loads():
        left_q = qn - QA
        return (
            pltpu.make_async_copy(wq_hbm.at[:, pl.ds(QA, left_q)], gu_buf.at[0, :, pl.ds(0, left_q)], w_sem.at[1]),
            pltpu.make_async_copy(wk_hbm, gu_buf.at[0, :, pl.ds(left_q, hd)], w_sem.at[2]),
            pltpu.make_async_copy(wv_hbm, gu_buf.at[0, :, pl.ds(left_q + hd, hd)], w_sem.at[3]),
        )

    x_copy(0).start()
    barrier = pltpu.get_barrier_semaphore()
    for dev in (right, left, sib):
        pl.semaphore_signal(barrier, inc=1, device_id={"tp": dev})
    pl.semaphore_wait(barrier, 3)
    ag1_own(0)
    wo_copy = pltpu.make_async_copy(wo_hbm, w_out, w_sem.at[4])
    for cp in (*qa_loads(), *qb_loads(), wo_copy):
        cp.start()
    shift[...] = jnp.zeros_like(shift)
    lax.fori_loop(0, n_chunks * R, table, 0)
    wo_copy.wait()

    def ready(c):
        ag_fin(0, c)
        for cp in (*att_loads(c, 0), *cache_loads(c, 0)):
            cp.start()

    def lead(i, carry):
        @pl.when(i == 0)
        def _():
            ag_fwd(0, 0)
            ag1_own(1)
            ag_far(0, 0)
            ready(0)

        @pl.when(i == 1)
        def _():
            ag_fwd(0, 1)
            ag1_own(2)

        @pl.when(i == R)
        def _():
            ag_far(0, 1)
            rs_pair(0, 0)
            ready(1)
            rs_half_load(0, 0)
            rs_half(0, 0)

        @pl.when(i == R + 1)
        def _():
            ag_fwd(0, 2)
            rs_relay_load(0, 0)
            rs_relay(0, 0)

        @pl.when(i == 2 * R)
        def _():
            ag_far(0, 2)
            rs_pair(0, 1)
            rs1_fin_load(0)
            rs1_fin(0)
            ready(2)
            rs_sent(0, 0)

        @pl.when(i == 2 * R + 1)
        def _():
            ag_fwd(1, 0)
            rs_half_load(0, 1)
            rs_half(0, 1)

        attend(lax.div(i, R), lax.rem(i, R))
        return carry

    lax.fori_loop(0, LEAD * R, lead, 0)
    ag_far(1, 0)
    rs_pair(0, 2)
    ag_fin(1, 0)
    h2_load(0).start()

    def gu_tile(j):
        slot = lax.rem(j, GU_SLOTS)

        @pl.when(j + GU_SLOTS - 1 < n_gu)
        def _():
            for cp in gu_copies(j + GU_SLOTS - 1, lax.rem(j + GU_SLOTS - 1, GU_SLOTS)):
                cp.start()

        for cp in gu_copies(j, slot):
            cp.wait()
        both = jnp.dot(h2v[...].reshape(n_dev * blk, width), gu_buf[slot], preferred_element_type=F32)
        gate, up = both[:, :GU], both[:, GU:]
        act[:, pl.ds(pl.multiple_of(j * GU, GU), GU)] = (jax.nn.silu(gate) * up).astype(BF)

    def dn_tile(j):
        slot = lax.rem(j, DN_SLOTS)

        @pl.when(j + 1 < n_dn)
        def _():
            dn_copy(j + 1, 1 - slot).start()

        dn_copy(j, slot).wait()
        tile = jnp.dot(act[...], dn_buf[slot], preferred_element_type=F32).astype(BF)
        pp[1, :, :, :, pl.ds(pl.multiple_of(j * DN, DN), DN)] = tile.reshape(n_chip, 2, blk, DN)

    def tiles(fn, part_idx, per):
        def one(i, carry):
            fn(part_idx * per + i)
            return carry

        lax.fori_loop(0, per, one, 0)

    last = n_chunks - 1
    done = (n_dn // DN_PARTS) * 3 * DN
    cuts = ((0, done, 0), (done, width - done, 1))

    def step(s, carry):
        nxt, att, old = s + 1, s + LEAD - 1, s - 1
        more = nxt < n_chunks
        has_att = (s > 0) & (att < n_chunks)

        def gu_part(k, carry):
            def at(when, cond, name, fn, chunk):
                @pl.when((k == when) & cond)
                def _():
                    fn(chunk)

            early = s == 0
            at(2, s > 0, "rs2_half", lambda c: rs_half(1, c), old)
            at(jnp.where(early, 1, 3), more, "rs1_relay", lambda c: rs_relay(0, c), nxt)
            at(5, s > 0, "rs2_relay", lambda c: rs_relay(1, c), old)
            at(jnp.where(early, 6, 8), more, "rs1_fin", rs1_fin, nxt)
            at(1, s > 0, "rs2_half_load", lambda c: rs_half_load(1, c), old)
            at(1, has_att, "ag1_fwd", lambda c: ag_fwd(0, c), att)
            at(jnp.where(early, 0, 2), more, "rs1_relay_load", lambda c: rs_relay_load(0, c), nxt)
            at(4, s > 0, "rs2_relay_load", lambda c: rs_relay_load(1, c), old)
            at(6, has_att, "ag1_far", lambda c: ag_far(0, c), att)
            at(7, has_att, "ready", ready, att)
            at(jnp.where(early, 5, 7), more, "rs1_fin_load", rs1_fin_load, nxt)

            @pl.when((k == GU_PARTS - 1) & has_att)
            def _():
                for cp in qa_loads():
                    cp.start()

            tiles(gu_tile, k, n_gu // GU_PARTS)
            return carry

        dn_copy(0, 0).start()
        h2_load(s).wait()
        lax.fori_loop(0, GU_PARTS, gu_part, 0)

        @pl.when(has_att)
        def _():
            for cp in qb_loads():
                cp.start()

        @pl.when(more & jnp.logical_not(has_att))
        def _():
            start_gu()

        @pl.when(more)
        def _():
            rs_sent(0, nxt)

        def att_step(r, carry):
            @pl.when((r == R - 1) & (s > 0))
            def _():
                rs2_fin_load(old)

            @pl.when(has_att)
            def _():
                attend(att, r)

            return carry

        lax.fori_loop(0, R, att_step, 0)

        @pl.when(has_att)
        def _():
            rs_pair(0, att)

        @pl.when(s > 0)
        def _():
            rs2_fin(old)

        def dn_part(k, carry):
            def at(when, cond, name, fn, chunk):
                @pl.when((k == when) & cond)
                def _():
                    fn(chunk)

            soon = has_att | (s == 0)

            def gathered(c):
                ag_fin(1, c)
                h2_load(c).start()

            at(2, att < n_chunks, "rs1_half", lambda c: rs_half(0, c), att)
            at(1, att < n_chunks, "rs1_half_load", lambda c: rs_half_load(0, c), att)
            at(jnp.where(soon, 0, 3), more, "ag2_fwd", lambda c: ag_fwd(1, c), nxt)
            at(0, att + 1 < n_chunks, "ag1_own", ag1_own, att + 1)
            at(jnp.where(has_att, 3, 2), more & soon, "ag2_far", lambda c: ag_far(1, c), nxt)
            at(4, more & soon, "ag2_fin", gathered, nxt)
            at(3, s == last, "tail_pair", lambda c: rs_pair(1, c, cuts[0]), s)
            at(4, s == last, "tail_half_load", lambda c: rs_half_load(1, c, cuts[0]), s)
            at(4, s == last, "tail_half", lambda c: rs_half(1, c, cuts[0]), s)
            tiles(dn_tile, k, n_dn // DN_PARTS)
            return carry

        lax.fori_loop(0, DN_PARTS, dn_part, 0)

        @pl.when(more & jnp.logical_not(has_att | (s == 0)))
        def _():
            ag_far(1, nxt)
            ag_fin(1, nxt)
            h2_load(nxt).start()

        @pl.when(more)
        def _():
            rs_pair(1, s)

        return carry

    lax.fori_loop(0, n_chunks, step, 0)

    rs_pair(1, last, cuts[1])
    x1_store(last).wait()
    out_store(last - 1).wait()
    xend_copy(last).start()
    rs_half_load(1, last, cuts[1])
    rs_half(1, last, cuts[1])
    for cut in cuts:
        rs_relay_load(1, last, cut)
        rs_relay(1, last, cut)
    xend_copy(last).wait()
    for cut in cuts:
        rs_fin_load(1, last, cut)
        rs2_add(last, cut)
    out_store(last).start()
    for cut in cuts:
        rs_sent(1, last, cut)
    out_store(last).wait()


def fused_layer(x, freq, bias, k_cache, v_cache, prefix, valid, g_attn, g_mlp, w_q, w_k, w_v, w_o, w_gate, w_up, w_down, n_dev):
    n_req, rows, width = x.shape
    n_chunks, blk = n_req // R, R * rows
    slots, hd = k_cache.shape[1:]
    tokens, qn, ffn = n_dev * rows, w_q.shape[1], w_gate.shape[1]
    n_chip = n_dev // 2
    hbm, smem, vmem = (pl.BlockSpec(memory_space=m) for m in (pl.ANY, pltpu.SMEM, pltpu.VMEM))
    chunked = lambda *s: jax.ShapeDtypeStruct((n_chunks, *s, width), BF)
    out_shape = [
        chunked(blk),
        jax.ShapeDtypeStruct(k_cache.shape, BF),
        jax.ShapeDtypeStruct(v_cache.shape, BF),
        chunked(n_dev, blk),
        chunked(n_dev, blk),
        chunked(n_chip, blk),
        chunked(n_chip, blk),
        chunked(2, rows),
        chunked(2, rows),
        chunked(2, blk),
        chunked(2, blk),
        chunked(blk),
        jax.ShapeDtypeStruct((n_req, tokens, hd), F32),
    ]
    dma = lambda *s: pltpu.SemaphoreType.DMA(s)
    rows_buf = pltpu.VMEM((blk, width), BF)
    scratch = [
        pltpu.VMEM((qn, width), BF),
        pltpu.VMEM((GU_SLOTS, width, 2 * GU), BF),
        pltpu.VMEM((DN_SLOTS, ffn, DN), BF),
        pltpu.VMEM((n_dev, blk, width), BF),
        pltpu.VMEM((n_dev, rows, width), BF),
        pltpu.VMEM((n_dev * blk, ffn), BF),
        pltpu.VMEM((2, n_chip, 2, blk, width), BF),
        *[rows_buf] * 6,
        pltpu.VMEM((2, blk, width), BF),
        pltpu.VMEM((1, blk, width), BF),
        *[pltpu.VMEM((slots, hd), BF)] * 2,
        pltpu.VMEM((2 * slots, hd), F32),
        pltpu.VMEM((tokens, hd), F32),
        pltpu.VMEM((2, tokens, slots), F32),
        dma(2, n_chunks, 9),
        dma(2, n_chunks, 9),
        dma(2, n_chunks + 1, 8),
        dma(2, n_chunks + 1, 8),
        dma(4),
        dma(3),
        dma(2, 2),
        dma(2),
        dma(4),
        dma(2),
        dma(GU_SLOTS, 2),
        dma(DN_SLOTS),
        dma(5),
        pltpu.SemaphoreType.DMA,
    ]
    res = pl.pallas_call(
        layer_kernel,
        in_specs=[smem, smem, vmem, vmem, vmem, vmem] + [hbm] * 10,
        out_specs=[hbm] * len(out_shape),
        out_shape=out_shape,
        scratch_shapes=scratch,
        compiler_params=pltpu.CompilerParams(vmem_limit_bytes=67_000_000, collective_id=0, has_side_effects=True),
        name="layer",
    )(prefix, valid, bias, g_attn[None], g_mlp[None], freq, x.reshape(n_chunks, blk, width), k_cache, v_cache, w_q, w_k, w_v, w_o, w_gate, w_up, w_down)
    return res[0].reshape(x.shape), res[1], res[2]


def solution(mesh):
    row_spec = P("dp", "tp", None)
    cache_spec = P("dp", None, "tp", None)
    req_spec = P("dp")
    rep_spec = P(None)
    col_spec = P(None, "tp")
    bias_spec = P("tp")
    down_spec = P("tp", None)
    n_dev = mesh.shape["tp"]

    def layer(x_rows, k_cache, v_cache, prefix, valid, g_attn, w_q, b_q, w_k, b_k, w_v, b_v, w_o, g_mlp, w_gate, w_up, w_down):
        n_req, rows, _ = x_rows.shape
        slots, hd = k_cache.shape[1], k_cache.shape[3]
        keys, vals = k_cache.reshape(n_req, slots, hd), v_cache.reshape(n_req, slots, hd)
        inv_freq = ROPE_THETA ** (-np.arange(0, hd, 2) / hd)
        freq = jnp.asarray(np.tile(inv_freq, 2)[None], F32)
        bias = jnp.concatenate([b_q, b_k, b_v])[None]
        out, k_out, v_out = fused_layer(x_rows, freq, bias, keys, vals, prefix, valid, g_attn, g_mlp, w_q, w_k, w_v, w_o, w_gate, w_up, w_down, n_dev)
        return out, k_out.reshape(k_cache.shape), v_out.reshape(v_cache.shape)

    in_specs = (row_spec, cache_spec, cache_spec, req_spec, req_spec, rep_spec, col_spec, bias_spec, col_spec, bias_spec, col_spec, bias_spec, down_spec, rep_spec, col_spec, col_spec, down_spec)
    return jax.shard_map(layer, mesh=mesh, in_specs=in_specs, out_specs=(row_spec, cache_spec, cache_spec), check_vma=False)
```

```python
import functools

import jax
import jax.numpy as jnp
import numpy as np
from jax import lax
from jax.experimental import pallas as pl
from jax.experimental.pallas import tpu as pltpu
from jax.sharding import PartitionSpec as P

ROPE_THETA = 1.0e6
NORM_EPS = 1.0e-6
LOG2_E = 1.4426950408889634
BF = jnp.bfloat16
F32 = jnp.float32
R = 2
GU = 384
DN = 512
GU_SLOTS, DN_SLOTS = 2, 2
QA = 512
ATT, MLP = 0, 1
SUB = 16
LEAD = 3

GU_PARTS, DN_PARTS = 9, 5


def layer_kernel(
    p_ref, c_ref, bq_ref, bk_ref, bv_ref, g1_ref, g2_ref, freq_ref, x_hbm, kc_hbm, vc_hbm, wq_hbm, wk_hbm, wv_hbm, wo_hbm, wg_hbm, wu_hbm, wd_hbm,
    out_hbm, ko_hbm, vo_hbm, h1_hbm, h2_hbm, sb1_hbm, sb2_hbm, rb1_hbm, rb2_hbm, fb1_hbm, fb2_hbm, x1_hbm, cs_hbm,
    w_out, gu_buf, dn_buf, h2v, h1v, act, pp, t_a, t_b, t_c, xin, xmid, xend, hb1, hb2, kb, vb, shift, csv, sbuf,
    ag_s, ag_r, rs_s, rs_r, tmp_sem, x_sem, h_sem, st_sem, at_sem, kv_sem, gu_sem, dn_sem, w_sem, h2_sem,
):
    n_chunks, blk, width = x_hbm.shape
    half = blk // R
    tokens, hd = cs_hbm.shape[1], cs_hbm.shape[2]
    slots = kc_hbm.shape[1]
    qn = w_out.shape[0]
    ffn = act.shape[1]
    n_gu, n_dn = ffn // GU, width // DN
    n_dev = h1_hbm.shape[1]
    n_chip = n_dev // 2

    me = lax.axis_index("tp")
    core = lax.rem(me, 2)
    chip = lax.div(me, 2)
    chips = [lax.rem(chip + 2, n_chip), lax.rem(chip + 1, n_chip), lax.rem(chip + 3, n_chip), chip]
    far, right_chip, left_chip, _ = chips
    right, left, sib = 2 * right_chip + core, 2 * left_chip + core, me + 1 - 2 * core

    hbufs, gains = (hb1, hb2), (g1_ref, g2_ref)
    h_all = (h1_hbm, h2_hbm)
    sbs, rbs, fbs = (sb1_hbm, sb2_hbm), (rb1_hbm, rb2_hbm), (fb1_hbm, fb2_hbm)

    def p_slot(s, c):
        return jnp.where(c == n_chunks - 2, 0, 1) if s else jnp.where(c == 1, 1, 0)

    def part(s, c):
        return pp.at[p_slot(s, c)]

    def h_slot(s, c):
        return 0 if s else lax.rem(c, 2)

    def ag(s, c, k):
        h = h_all[s]
        lo, hi = pl.ds(0, half), pl.ds(half, half)
        lt, rt, ft = 2 * left_chip + core, 2 * right_chip + core, 2 * far + core
        own = hbufs[s].at[h_slot(s, c)]
        src, dst, dev = [
            (own.at[lo], h.at[c, me, lo], right),
            (own.at[hi], h.at[c, me, hi], right),
            (own.at[hi], h.at[c, me, hi], left),
            (own.at[lo], h.at[c, me, lo], left),
            (own, h.at[c, me], sib),
            (h.at[c, lt, lo], h.at[c, lt, lo], right),
            (h.at[c, rt, hi], h.at[c, rt, hi], left),
            (h.at[c, lt], h.at[c, lt], sib),
            (h.at[c, rt], h.at[c, rt], sib),
            (h.at[c, ft, lo], h.at[c, ft, lo], sib),
            (h.at[c, ft, hi], h.at[c, ft, hi], sib),
        ][k]
        return pltpu.make_async_remote_copy(src, dst, ag_s.at[s, lax.rem(c, 2), k], ag_r.at[s, c, k], device_id={"tp": dev})

    def rs(s, c, k, cut=None):
        col, got = (pl.ds(0, width), c) if cut is None else (pl.ds(*cut[:2]), n_chunks - 1 + cut[2])
        sent = (s, lax.rem(c, 2)) if cut is None or cut[2] == 0 else (0, cut[2] - 1)
        p, lo, hi = part(s, c), pl.ds(0, half), pl.ds(half, half)
        all_rows = pl.ds(0, blk)
        if k < 4:
            src, dst, dev = p.at[chips[k], 1 - core, all_rows, col], sbs[s].at[c, k, all_rows, col], sib
        else:
            src, dst, dev = [
                (p.at[far, core, lo, col], rbs[s].at[c, 0, pl.ds(0, half), col], right),
                (p.at[far, core, hi, col], rbs[s].at[c, 1, pl.ds(0, half), col], left),
                (p.at[right_chip, core, hi, col], fbs[s].at[c, 0, hi, col], right),
                (p.at[left_chip, core, lo, col], fbs[s].at[c, 1, lo, col], left),
                (p.at[right_chip, core, lo, col], fbs[s].at[c, 0, lo, col], right),
                (p.at[left_chip, core, hi, col], fbs[s].at[c, 1, hi, col], left),
            ][k - 4]
        return pltpu.make_async_remote_copy(src, dst, rs_s.at[*sent, k], rs_r.at[s, got, k], device_id={"tp": dev})

    def by_rows(rows, fn):
        def step(i, carry):
            fn(pl.ds(pl.multiple_of(i * SUB, SUB), SUB))
            return carry

        lax.fori_loop(0, rows // SUB, step, 0)

    def f32(v):
        return v.astype(F32)

    def row(v):
        return f32(v).reshape(1, v.shape[0])

    def normed(wide, gain):
        inv_rms = lax.rsqrt(jnp.mean(wide * wide, axis=-1, keepdims=True) + NORM_EPS)
        return (wide * inv_rms * row(gain[...])).astype(BF)

    def own_copy(s, c):
        slot = h_slot(s, c)
        return pltpu.make_async_copy(hbufs[s].at[slot], h_all[s].at[c, me], h_sem.at[s, slot])

    def x_copy(c):
        return pltpu.make_async_copy(x_hbm.at[c], xin, x_sem.at[0])

    def ag_send(s, c):
        own_copy(s, c).start()
        for k in (0, 2, 1, 3, 4):
            ag(s, c, k).start()

    def ag1_own(c):
        x_copy(c).wait()

        def fn(rows):
            hb1[h_slot(ATT, c), rows, :] = normed(f32(xin[rows, :]), g1_ref)

        by_rows(blk, fn)
        ag_send(ATT, c)

        @pl.when(c + 1 < n_chunks)
        def _():
            x_copy(c + 1).start()

    def ag_fwd(s, c):
        ag(s, c, 0).wait_recv()
        ag(s, c, 5).start()
        ag(s, c, 2).wait_recv()
        ag(s, c, 6).start()

    def ag_far(s, c):
        for got, send in ((1, 7), (3, 8), (5, 9), (6, 10)):
            ag(s, c, got).wait_recv()
            ag(s, c, send).start()

    def ag_fin(s, c):
        for k in (4, 7, 8, 9, 10):
            ag(s, c, k).wait_recv()
        for k in range(11):
            ag(s, c, k).wait_send()
        own_copy(s, c).wait()

    def rs_pair(s, c, cut=None):
        for k in range(4):
            rs(s, c, k, cut).start()

    def loads(srcs, cut):
        col, row_idx = (pl.ds(0, width), 0) if cut is None else (pl.ds(*cut[:2]), cut[2])
        return [pltpu.make_async_copy(src.at[:, col], dst.at[:, col], tmp_sem.at[row_idx, i]) for i, (src, dst) in enumerate(srcs)]

    lo_rows, hi_rows = pl.ds(0, half), pl.ds(half, half)

    def half_loads(s, c, cut):
        sb = sbs[s]
        return loads([(sb.at[c, 0], t_a), (sb.at[c, 1, hi_rows], t_b.at[hi_rows]), (sb.at[c, 2, lo_rows], t_b.at[lo_rows])], cut)

    def rs_half_load(s, c, cut=None):
        for k, cp in enumerate(half_loads(s, c, cut)):
            rs(s, c, k, cut).wait_recv()
            cp.start()

    def halves(fn):
        def step(i, carry):
            fn(pl.ds(pl.multiple_of(i * SUB, SUB), SUB), pl.ds(pl.multiple_of(half + i * SUB, SUB), SUB))
            return carry

        lax.fori_loop(0, half // SUB, step, 0)

    def rs_half(s, c, cut=None, eager=False):
        for cp in half_loads(s, c, cut):
            cp.wait()
        p, col = part(s, c), slice(None) if cut is None else pl.ds(*cut[:2])

        def fn(lo, hi):
            for rows in (lo, hi):
                p[far, core, rows, col] = (f32(p[far, core, rows, col]) + f32(t_a[rows, col])).astype(BF)
            p[right_chip, core, hi, col] = (f32(p[right_chip, core, hi, col]) + f32(t_b[hi, col])).astype(BF)
            p[left_chip, core, lo, col] = (f32(p[left_chip, core, lo, col]) + f32(t_b[lo, col])).astype(BF)

        halves(fn)
        for k in range(4, 8 if eager else 6):
            rs(s, c, k, cut).start()

    def relay_loads(s, c, cut):
        sb, rb = sbs[s], rbs[s]
        return loads(
            [(sb.at[c, 1, lo_rows], t_a.at[lo_rows]), (sb.at[c, 2, hi_rows], t_a.at[hi_rows]), (rb.at[c, 0], t_c.at[lo_rows]), (rb.at[c, 1], t_c.at[hi_rows])], cut
        )

    def rs_relay_load(s, c, cut=None):
        for k in (4, 5):
            rs(s, c, k, cut).wait_recv()
        for cp in relay_loads(s, c, cut):
            cp.start()

    def rs_relay(s, c, cut=None, eager=False):
        for cp in relay_loads(s, c, cut):
            cp.wait()
        p, col = part(s, c), slice(None) if cut is None else pl.ds(*cut[:2])

        def fn(lo, hi):
            p[right_chip, core, lo, col] = (f32(p[right_chip, core, lo, col]) + f32(t_a[lo, col]) + f32(t_c[lo, col])).astype(BF)
            p[left_chip, core, hi, col] = (f32(p[left_chip, core, hi, col]) + f32(t_a[hi, col]) + f32(t_c[hi, col])).astype(BF)

        halves(fn)
        for k in (8, 9) if eager else (8, 9, 6, 7):
            rs(s, c, k, cut).start()

    def fin_loads(s, c, cut):
        return loads([(sbs[s].at[c, 3], t_a), (fbs[s].at[c, 0], t_b), (fbs[s].at[c, 1], t_c)], cut)

    def rs_fin_load(s, c, cut=None):
        for k in (3, 6, 7, 8, 9):
            rs(s, c, k, cut).wait_recv()
        for cp in fin_loads(s, c, cut):
            cp.start()

    def rs_total(s, c, rows, col=slice(None)):
        p = part(s, c)
        return (f32(p[chip, core, rows, col]) + f32(t_a[rows, col]) + f32(t_b[rows, col]) + f32(t_c[rows, col])).astype(BF)

    def rs_sent(s, c, cut=None):
        for k in range(10):
            rs(s, c, k, cut).wait_send()

    def xmid_copy(c):
        return pltpu.make_async_copy(x_hbm.at[c], xmid, x_sem.at[1])

    def x1_store(c):
        return pltpu.make_async_copy(xmid, x1_hbm.at[c], st_sem.at[0])

    def xend_copy(c):
        return pltpu.make_async_copy(x1_hbm.at[c], xend, x_sem.at[2])

    def out_store(c):
        return pltpu.make_async_copy(xend, out_hbm.at[c], st_sem.at[1])

    def rs1_fin_load(c):
        @pl.when(c > 0)
        def _():
            x1_store(c - 1).wait()

        xmid_copy(c).start()
        rs_fin_load(ATT, c)

    def rs1_fin(c):
        for cp in fin_loads(ATT, c, None):
            cp.wait()
        xmid_copy(c).wait()

        def fn(rows):
            mid = (f32(xmid[rows, :]) + f32(rs_total(ATT, c, rows))).astype(BF)
            xmid[rows, :] = mid
            hb2[0, rows, :] = normed(f32(mid), g2_ref)

        by_rows(blk, fn)
        x1_store(c).start()
        ag_send(MLP, c)

    def rs2_fin_load(c):
        @pl.when(c > 0)
        def _():
            out_store(c - 1).wait()

        xend_copy(c).start()
        rs_fin_load(MLP, c)

    def rs2_add(c, cut=None):
        for cp in fin_loads(MLP, c, cut):
            cp.wait()
        col = slice(None) if cut is None else pl.ds(*cut[:2])

        def fn(rows):
            xend[rows, col] = (f32(xend[rows, col]) + f32(rs_total(MLP, c, rows, col))).astype(BF)

        by_rows(blk, fn)

    def rs2_fin(c):
        xend_copy(c).wait()
        rs2_add(c)
        out_store(c).start()
        rs_sent(MLP, c)

    def att_loads(a, r):
        return (
            pltpu.make_async_copy(h1_hbm.at[a, :, pl.ds(pl.multiple_of(r * half, half), half)], h1v, at_sem.at[0]),
            pltpu.make_async_copy(cs_hbm.at[a * R + r], csv, at_sem.at[3]),
        )

    def cache_loads(a, r):
        return (
            pltpu.make_async_copy(kc_hbm.at[a * R + r], kb, at_sem.at[1]),
            pltpu.make_async_copy(vc_hbm.at[a * R + r], vb, at_sem.at[2]),
        )

    def table(req, carry):
        pos = p_ref[req] + lax.broadcasted_iota(jnp.int32, (tokens, hd), 0)
        angles = f32(pos) * freq_ref[...]
        first = lax.broadcasted_iota(jnp.int32, (tokens, hd), 1) < hd // 2
        csv[...] = jnp.where(first, jnp.cos(angles), jnp.sin(angles))
        cp = pltpu.make_async_copy(csv, cs_hbm.at[req], at_sem.at[3])
        cp.start()
        cp.wait()
        return carry

    def attend(a, r):
        req = a * R + r
        p_out = part(ATT, a)
        for cp in (*att_loads(a, r), *cache_loads(a, r)):
            cp.wait()
        fresh = (r == 0) & ((a == 0) | (a >= LEAD))
        h = h1v[...].reshape(tokens, width)

        def project(cps, slot, bias):
            @pl.when(fresh)
            def _():
                for cp in cps:
                    cp.wait()

            total = jnp.dot(h, gu_buf[slot, :, 0 : bias.shape[1]], preferred_element_type=F32)
            return f32((total + bias).astype(BF))

        some_q = project(qa_loads(), 1, row(bq_ref[0:QA]))
        rest = project(qb_loads(), 0, jnp.concatenate([row(bq_ref[QA:qn]), row(bk_ref[...]), row(bv_ref[...])], axis=1))
        p, c = p_ref[req], c_ref[req]
        cs = csv[...]
        sc = pltpu.roll(cs, hd // 2, 1)
        first = lax.broadcasted_iota(jnp.int32, (tokens, hd), 1) < hd // 2
        cos, sin = jnp.where(first, cs, sc), jnp.where(first, -sc, cs)

        def head(j):
            return some_q[:, j * hd : (j + 1) * hd] if j * hd < QA else rest[:, j * hd - QA : (j + 1) * hd - QA]

        def rope(v):
            return v * cos + pltpu.roll(v, hd // 2, 1) * sin

        n_heads, groups = qn // hd, tokens // blk
        for j in range(n_heads):
            h2v[0:groups, :, j * hd : (j + 1) * hd] = rope(head(j)).astype(BF).reshape(groups, blk, hd)
        slot = lax.broadcasted_iota(jnp.int32, (slots, hd), 0)
        new = (slot >= p) & (slot < p + c)
        shift[slots : slots + tokens, :] = rope(head(n_heads))
        kb[...] = jnp.where(new, shift[pl.ds(slots - p, slots), :], f32(kb[...])).astype(BF)
        shift[slots : slots + tokens, :] = head(n_heads + 1)
        vb[...] = jnp.where(new, shift[pl.ds(slots - p, slots), :], f32(vb[...])).astype(BF)
        stores = (pltpu.make_async_copy(kb, ko_hbm.at[req], kv_sem.at[0]), pltpu.make_async_copy(vb, vo_hbm.at[req], kv_sem.at[1]))
        for cp in stores:
            cp.start()

        @pl.when(r + 1 < R)
        def _():
            for cp in att_loads(a, r + 1):
                cp.start()

        @pl.when((r == R - 1) & (a >= LEAD - 1))
        def _():
            start_gu()

        def scores(j):
            q = h2v[0:groups, :, j * hd : (j + 1) * hd].reshape(tokens, hd)
            return lax.dot_general(q, kb[...], (((1,), (1,)), ((), ())), preferred_element_type=F32)

        limit = p + jnp.minimum(lax.broadcasted_iota(jnp.int32, (tokens, slots), 0), c - 1)
        visible = lax.broadcasted_iota(jnp.int32, (tokens, slots), 1) <= limit
        sbuf[0] = scores(0)
        for j in range(n_heads):
            if j + 1 < n_heads:
                sbuf[(j + 1) % 2] = scores(j + 1)
            masked = jnp.where(visible, sbuf[j % 2], -1.0e30)
            expd = jnp.exp2((masked - jnp.max(masked, axis=1, keepdims=True)) * (hd**-0.5 * LOG2_E))
            probs = (expd * (1.0 / jnp.sum(expd, axis=1, keepdims=True))).astype(BF)
            mixed = jnp.dot(probs, vb[...], preferred_element_type=F32).astype(BF)
            h2v[groups : 2 * groups, :, j * hd : (j + 1) * hd] = mixed.reshape(groups, blk, hd)
        for cp in stores:
            cp.wait()

        @pl.when(r + 1 < R)
        def _():
            for cp in cache_loads(a, r + 1):
                cp.start()

        heads = h2v[groups : 2 * groups, :, 0:qn].reshape(tokens, qn)
        out = jnp.dot(heads, w_out[...], preferred_element_type=F32).astype(BF)
        p_out[:, :, pl.ds(pl.multiple_of(r * half, half), half), :] = out.reshape(n_chip, 2, half, width)

    def gu_copies(tile, slot):
        cols = pl.ds(pl.multiple_of(tile * GU, GU), GU)
        return (
            pltpu.make_async_copy(wg_hbm.at[:, cols], gu_buf.at[slot, :, pl.ds(0, GU)], gu_sem.at[slot, 0]),
            pltpu.make_async_copy(wu_hbm.at[:, cols], gu_buf.at[slot, :, pl.ds(GU, GU)], gu_sem.at[slot, 1]),
        )

    def dn_copy(tile, slot):
        cols = pl.ds(pl.multiple_of(tile * DN, DN), DN)
        return pltpu.make_async_copy(wd_hbm.at[:, cols], dn_buf.at[slot], dn_sem.at[slot])

    def h2_load(c):
        return pltpu.make_async_copy(h2_hbm.at[c], h2v, h2_sem)

    def start_gu():
        for tile in range(GU_SLOTS - 1):
            for cp in gu_copies(tile, tile):
                cp.start()

    def qa_loads():
        return (pltpu.make_async_copy(wq_hbm.at[:, pl.ds(0, QA)], gu_buf.at[1, :, pl.ds(0, QA)], w_sem.at[0]),)

    def qb_loads():
        left_q = qn - QA
        return (
            pltpu.make_async_copy(wq_hbm.at[:, pl.ds(QA, left_q)], gu_buf.at[0, :, pl.ds(0, left_q)], w_sem.at[1]),
            pltpu.make_async_copy(wk_hbm, gu_buf.at[0, :, pl.ds(left_q, hd)], w_sem.at[2]),
            pltpu.make_async_copy(wv_hbm, gu_buf.at[0, :, pl.ds(left_q + hd, hd)], w_sem.at[3]),
        )

    x_copy(0).start()
    barrier = pltpu.get_barrier_semaphore()
    for dev in (right, left, sib):
        pl.semaphore_signal(barrier, inc=1, device_id={"tp": dev})
    pl.semaphore_wait(barrier, 3)
    ag1_own(0)
    wo_copy = pltpu.make_async_copy(wo_hbm, w_out, w_sem.at[4])
    for cp in (*qa_loads(), *qb_loads(), wo_copy):
        cp.start()
    shift[...] = jnp.zeros_like(shift)
    lax.fori_loop(0, 2 * n_chunks * R // 3, table, 0)
    ag_fwd(ATT, 0)
    lax.fori_loop(2 * n_chunks * R // 3, n_chunks * R, table, 0)
    wo_copy.wait()

    def ready(c):
        ag_fin(ATT, c)
        for cp in (*att_loads(c, 0), *cache_loads(c, 0)):
            cp.start()

    def lead(i, carry):
        @pl.when(i == 0)
        def _():
            ag1_own(1)
            ag_far(ATT, 0)
            ready(0)

        @pl.when(i == 1)
        def _():
            ag_fwd(ATT, 1)
            ag1_own(2)

        @pl.when(i == R)
        def _():
            ag_far(ATT, 1)
            rs_pair(ATT, 0)
            ready(1)
            rs_half_load(ATT, 0)
            rs_half(ATT, 0, eager=True)

        @pl.when(i == R + 1)
        def _():
            rs_relay_load(ATT, 0)
            rs_relay(ATT, 0, eager=True)
            ag_fwd(ATT, 2)

        @pl.when(i == 2 * R)
        def _():
            rs_pair(ATT, 1)
            rs1_fin_load(0)
            rs1_fin(0)
            ag_far(ATT, 2)
            ready(2)
            rs_sent(ATT, 0)

        @pl.when(i == 2 * R + 1)
        def _():
            ag_fwd(MLP, 0)
            rs_half_load(ATT, 1)
            rs_half(ATT, 1)

        attend(lax.div(i, R), lax.rem(i, R))
        return carry

    lax.fori_loop(0, LEAD * R, lead, 0)
    ag_far(MLP, 0)
    rs_pair(ATT, 2)
    ag_fin(MLP, 0)
    h2_load(0).start()

    last = n_chunks - 1
    unit = (n_dn // DN_PARTS) * DN
    cuts = ((0, 2 * unit, 0), (2 * unit, 2 * unit, 1), (4 * unit, width - 4 * unit, 2))

    def gu_tile(j):
        slot = lax.rem(j, GU_SLOTS)

        @pl.when(j + GU_SLOTS - 1 < n_gu)
        def _():
            for cp in gu_copies(j + GU_SLOTS - 1, lax.rem(j + GU_SLOTS - 1, GU_SLOTS)):
                cp.start()

        for cp in gu_copies(j, slot):
            cp.wait()
        both = jnp.dot(h2v[...].reshape(n_dev * blk, width), gu_buf[slot], preferred_element_type=F32)
        gate, up = both[:, :GU], both[:, GU:]
        act[:, pl.ds(pl.multiple_of(j * GU, GU), GU)] = (jax.nn.silu(gate) * up).astype(BF)

    def dn_tile(s, j):
        slot = lax.rem(j, DN_SLOTS)

        @pl.when((s == last) & (j == n_dn - 1))
        def _():
            rs_relay_load(MLP, last, cuts[0])
            rs_half_load(MLP, last, cuts[1])
            rs_relay(MLP, last, cuts[0], True)
            rs_half(MLP, last, cuts[1], True)

        @pl.when(j + 1 < n_dn)
        def _():
            dn_copy(j + 1, 1 - slot).start()

        dn_copy(j, slot).wait()
        tile = jnp.dot(act[...], dn_buf[slot], preferred_element_type=F32).astype(BF)
        pp[p_slot(MLP, s), :, :, :, pl.ds(pl.multiple_of(j * DN, DN), DN)] = tile.reshape(n_chip, 2, blk, DN)

    def tiles(fn, part_idx, per):
        def one(i, carry):
            fn(part_idx * per + i)
            return carry

        lax.fori_loop(0, per, one, 0)

    def step(s, carry):
        nxt, att, old = s + 1, s + LEAD - 1, s - 1
        more = nxt < n_chunks
        has_att = (s > 0) & (att < n_chunks)

        def gu_part(k, carry):
            def at(when, cond, name, fn, chunk):
                @pl.when((k == when) & cond)
                def _():
                    fn(chunk)

            early, pen = s == 0, s == last - 1
            pick = lambda att_at, pen_at, else_at: jnp.where(has_att, att_at, jnp.where(pen, pen_at, else_at))
            at(0, pen, "rs1_relay", lambda c: rs_relay(ATT, c), nxt)
            at(2, s > 0, "rs2_half", lambda c: rs_half(MLP, c), old)
            at(jnp.where(early, 1, 3), s < last - 1, "rs1_relay", lambda c: rs_relay(ATT, c), nxt)
            at(8, pen, "ag2_fwd", lambda c: ag_fwd(MLP, c), nxt)
            at(pick(6, 8, 5), s > 0, "rs2_relay", lambda c: rs_relay(MLP, c), old)
            at(pick(-1, 5, 6), more, "rs1_fin", rs1_fin, nxt)
            at(1, s > 0, "rs2_half_load", lambda c: rs_half_load(MLP, c), old)
            at(1, has_att, "ag1_fwd", lambda c: ag_fwd(ATT, c), att)
            at(jnp.where(early, 0, 2), s < last - 1, "rs1_relay_load", lambda c: rs_relay_load(ATT, c), nxt)
            at(pick(5, 7, 4), s > 0, "rs2_relay_load", lambda c: rs_relay_load(MLP, c), old)
            at(6, has_att, "ag1_far", lambda c: ag_far(ATT, c), att)
            at(7, has_att, "ready", ready, att)
            at(pick(8, 4, 5), more, "rs1_fin_load", rs1_fin_load, nxt)

            @pl.when((k == GU_PARTS - 1) & has_att)
            def _():
                for cp in qa_loads():
                    cp.start()

            tiles(gu_tile, k, n_gu // GU_PARTS)
            return carry

        dn_copy(0, 0).start()
        h2_load(s).wait()
        lax.fori_loop(0, GU_PARTS, gu_part, 0)

        @pl.when(has_att)
        def _():
            for cp in qb_loads():
                cp.start()
            rs1_fin(nxt)

        @pl.when(more & jnp.logical_not(has_att))
        def _():
            start_gu()

        @pl.when(more)
        def _():
            rs_sent(ATT, nxt)

        def att_step(r, carry):
            @pl.when((r == R - 1) & has_att)
            def _():
                rs2_fin_load(old)

            @pl.when(has_att)
            def _():
                attend(att, r)

            return carry

        lax.fori_loop(0, R, att_step, 0)

        @pl.when(has_att)
        def _():
            rs_pair(ATT, att)
            rs2_fin(old)

        def dn_part(k, carry):
            def at(when, cond, name, fn, chunk):
                @pl.when((k == when) & cond)
                def _():
                    fn(chunk)

            pen = s == last - 1
            pick = lambda att_at, pen_at, else_at: jnp.where(has_att, att_at, jnp.where(pen, pen_at, else_at))

            def gathered(c):
                ag_fin(MLP, c)
                h2_load(c).start(priority=1)

            at(2, s == last, "rs2_fin", rs2_fin, old)
            at(2, att < n_chunks, "rs1_half", lambda c: rs_half(ATT, c), att)
            at(1, att < n_chunks, "rs1_half_load", lambda c: rs_half_load(ATT, c), att)
            at(0, more & jnp.logical_not(pen), "ag2_fwd", lambda c: ag_fwd(MLP, c), nxt)
            at(0, att + 1 < n_chunks, "ag1_own", ag1_own, att + 1)
            at(pick(3, 1, 2), more, "ag2_far", lambda c: ag_far(MLP, c), nxt)
            at(pick(4, 2, 4), more, "ag2_fin", gathered, nxt)
            at(4, s == last - 2, "rs1_relay_load", lambda c: rs_relay_load(ATT, c), att)
            at(jnp.where(pen, 4, 1), pen | (s == last), "rs2_fin_load", rs2_fin_load, old)
            at(2, s == last, "tail_pair", lambda c: rs_pair(MLP, c, cuts[0]), s)
            at(3, s == last, "tail_half_load", lambda c: rs_half_load(MLP, c, cuts[0]), s)
            at(3, s == last, "tail_half", lambda c: rs_half(MLP, c, cuts[0], True), s)
            at(4, s == last, "tail_pair", lambda c: rs_pair(MLP, c, cuts[1]), s)
            tiles(functools.partial(dn_tile, s), k, n_dn // DN_PARTS)
            return carry

        lax.fori_loop(0, DN_PARTS, dn_part, 0)

        @pl.when(s == last - 1)
        def _():
            rs2_fin(old)

        @pl.when(more)
        def _():
            rs_pair(MLP, s)

        return carry

    lax.fori_loop(0, n_chunks, step, 0)

    rs_pair(MLP, last, cuts[2])
    rs_half_load(MLP, last, cuts[2])
    rs_half(MLP, last, cuts[2], True)
    x1_store(last).wait()
    out_store(last - 1).wait()
    xend_copy(last).start()
    xend_copy(last).wait()
    rs_fin_load(MLP, last, cuts[0])
    rs_relay_load(MLP, last, cuts[1])
    rs_relay(MLP, last, cuts[1], True)
    rs2_add(last, cuts[0])
    rs_relay_load(MLP, last, cuts[2])
    rs_relay(MLP, last, cuts[2], True)
    for cut in cuts[1:]:
        rs_fin_load(MLP, last, cut)
        rs2_add(last, cut)
    out_store(last).start()
    for cut in cuts:
        rs_sent(MLP, last, cut)
    out_store(last).wait()


def fused_layer(x, freq, b_q, b_k, b_v, k_cache, v_cache, prefix, valid, g_attn, g_mlp, w_q, w_k, w_v, w_o, w_gate, w_up, w_down, n_dev):
    n_req, rows, width = x.shape
    n_chunks, blk = n_req // R, R * rows
    slots, hd = k_cache.shape[1:]
    tokens, qn, ffn = n_dev * rows, w_q.shape[1], w_gate.shape[1]
    n_chip = n_dev // 2
    hbm, smem, vmem = (pl.BlockSpec(memory_space=m) for m in (pl.ANY, pltpu.SMEM, pltpu.VMEM))
    chunked = lambda *s: jax.ShapeDtypeStruct((n_chunks, *s, width), BF)
    out_shape = [
        chunked(blk),
        jax.ShapeDtypeStruct(k_cache.shape, BF),
        jax.ShapeDtypeStruct(v_cache.shape, BF),
        chunked(n_dev, blk),
        chunked(n_dev, blk),
        chunked(n_chip, blk),
        chunked(n_chip, blk),
        chunked(2, rows),
        chunked(2, rows),
        chunked(2, blk),
        chunked(2, blk),
        chunked(blk),
        jax.ShapeDtypeStruct((n_req, tokens, hd), F32),
    ]
    dma = lambda *s: pltpu.SemaphoreType.DMA(s)
    rows_buf = pltpu.VMEM((blk, width), BF)
    scratch = [
        pltpu.VMEM((qn, width), BF),
        pltpu.VMEM((GU_SLOTS, width, 2 * GU), BF),
        pltpu.VMEM((DN_SLOTS, ffn, DN), BF),
        pltpu.VMEM((n_dev, blk, width), BF),
        pltpu.VMEM((n_dev, rows, width), BF),
        pltpu.VMEM((n_dev * blk, ffn), BF),
        pltpu.VMEM((2, n_chip, 2, blk, width), BF),
        *[rows_buf] * 6,
        pltpu.VMEM((2, blk, width), BF),
        pltpu.VMEM((1, blk, width), BF),
        *[pltpu.VMEM((slots, hd), BF)] * 2,
        pltpu.VMEM((2 * slots, hd), F32),
        pltpu.VMEM((tokens, hd), F32),
        pltpu.VMEM((2, tokens, slots), F32),
        dma(2, 2, 11),
        dma(2, n_chunks, 11),
        dma(2, 2, 10),
        dma(2, n_chunks + 2, 10),
        dma(3, 4),
        dma(3),
        dma(2, 2),
        dma(2),
        dma(4),
        dma(2),
        dma(GU_SLOTS, 2),
        dma(DN_SLOTS),
        dma(5),
        pltpu.SemaphoreType.DMA,
    ]
    res = pl.pallas_call(
        layer_kernel,
        in_specs=[smem, smem] + [vmem] * 6 + [hbm] * 10,
        out_specs=[hbm] * len(out_shape),
        out_shape=out_shape,
        scratch_shapes=scratch,
        compiler_params=pltpu.CompilerParams(vmem_limit_bytes=67_000_000, collective_id=0, has_side_effects=True),
        name="layer",
    )(prefix, valid, b_q, b_k, b_v, g_attn, g_mlp, freq, x.reshape(n_chunks, blk, width), k_cache, v_cache, w_q, w_k, w_v, w_o, w_gate, w_up, w_down)
    return res[0].reshape(x.shape), res[1], res[2]


def solution(mesh):
    row_spec = P("dp", "tp", None)
    cache_spec = P("dp", None, "tp", None)
    req_spec = P("dp")
    rep_spec = P(None)
    col_spec = P(None, "tp")
    bias_spec = P("tp")
    down_spec = P("tp", None)
    n_dev = mesh.shape["tp"]

    def layer(x_rows, k_cache, v_cache, prefix, valid, g_attn, w_q, b_q, w_k, b_k, w_v, b_v, w_o, g_mlp, w_gate, w_up, w_down):
        n_req, rows, _ = x_rows.shape
        slots, hd = k_cache.shape[1], k_cache.shape[3]
        keys, vals = k_cache.reshape(n_req, slots, hd), v_cache.reshape(n_req, slots, hd)
        inv_freq = ROPE_THETA ** (-np.arange(0, hd, 2) / hd)
        freq = jnp.asarray(np.tile(inv_freq, 2)[None], F32)
        out, k_out, v_out = fused_layer(x_rows, freq, b_q, b_k, b_v, keys, vals, prefix, valid, g_attn, g_mlp, w_q, w_k, w_v, w_o, w_gate, w_up, w_down, n_dev)
        return out, k_out.reshape(k_cache.shape), v_out.reshape(v_cache.shape)

    in_specs = (row_spec, cache_spec, cache_spec, req_spec, req_spec, rep_spec, col_spec, bias_spec, col_spec, bias_spec, col_spec, bias_spec, down_spec, rep_spec, col_spec, col_spec, down_spec)
    return jax.shard_map(layer, mesh=mesh, in_specs=in_specs, out_specs=(row_spec, cache_spec, cache_spec), check_vma=False)
```

```python
import functools

import jax
import jax.numpy as jnp
import numpy as np
from jax import lax
from jax.experimental import pallas as pl
from jax.experimental.pallas import tpu as pltpu
from jax.sharding import PartitionSpec as P

ROPE_THETA = 1.0e6
NORM_EPS = 1.0e-6
LOG2_E = 1.4426950408889634
BF = jnp.bfloat16
F32 = jnp.float32
R = 2
GU = 384
DN = 512
GU_SLOTS, DN_SLOTS = 2, 2
QA = 512
ATT, MLP = 0, 1
SUB = 16
LEAD = 3

GU_PARTS, DN_PARTS = 9, 5


def layer_kernel(
    p_ref, c_ref, bq_ref, bk_ref, bv_ref, g1_ref, g2_ref, freq_ref, x_hbm, kc_hbm, vc_hbm, wq_hbm, wk_hbm, wv_hbm, wo_hbm, wg_hbm, wu_hbm, wd_hbm,
    out_hbm, ko_hbm, vo_hbm, h1_hbm, h2_hbm, sb1_hbm, sb2_hbm, rb1_hbm, rb2_hbm, fb1_hbm, fb2_hbm, x1_hbm, cs_hbm,
    w_out, gu_buf, dn_buf, h2v, h1v, act, pp, t_a, t_b, t_c, xin, xmid, xend, hb1, hb2, kb, vb, shift, csv, sbuf,
    ag_s, ag_r, rs_s, rs_r, tmp_sem, x_sem, h_sem, st_sem, at_sem, kv_sem, gu_sem, dn_sem, w_sem, h2_sem,
):
    n_chunks, blk, width = x_hbm.shape
    half = blk // R
    tokens, hd = cs_hbm.shape[1], cs_hbm.shape[2]
    slots = kc_hbm.shape[1]
    qn = w_out.shape[0]
    ffn = act.shape[1]
    n_gu, n_dn = ffn // GU, width // DN
    n_dev = h1_hbm.shape[1]
    n_chip = n_dev // 2

    me = lax.axis_index("tp")
    core = lax.rem(me, 2)
    chip = lax.div(me, 2)
    chips = [lax.rem(chip + 2, n_chip), lax.rem(chip + 1, n_chip), lax.rem(chip + 3, n_chip), chip]
    far, right_chip, left_chip, _ = chips
    right, left, sib = 2 * right_chip + core, 2 * left_chip + core, me + 1 - 2 * core

    hbufs, gains = (hb1, hb2), (g1_ref, g2_ref)
    h_all = (h1_hbm, h2_hbm)
    sbs, rbs, fbs = (sb1_hbm, sb2_hbm), (rb1_hbm, rb2_hbm), (fb1_hbm, fb2_hbm)

    def p_slot(s, c):
        return jnp.where(c == n_chunks - 2, 0, 1) if s else jnp.where(c == 1, 1, 0)

    def part(s, c):
        return pp.at[p_slot(s, c)]

    def h_slot(s, c):
        return 0 if s else lax.rem(c, 2)

    def ag(s, c, k):
        h = h_all[s]
        lo, hi = pl.ds(0, half), pl.ds(half, half)
        lt, rt, ft = 2 * left_chip + core, 2 * right_chip + core, 2 * far + core
        own = hbufs[s].at[h_slot(s, c)]
        src, dst, dev = [
            (own.at[lo], h.at[c, me, lo], right),
            (own.at[hi], h.at[c, me, hi], right),
            (own.at[hi], h.at[c, me, hi], left),
            (own.at[lo], h.at[c, me, lo], left),
            (own, h.at[c, me], sib),
            (h.at[c, lt, lo], h.at[c, lt, lo], right),
            (h.at[c, rt, hi], h.at[c, rt, hi], left),
            (h.at[c, lt], h.at[c, lt], sib),
            (h.at[c, rt], h.at[c, rt], sib),
            (h.at[c, ft, lo], h.at[c, ft, lo], sib),
            (h.at[c, ft, hi], h.at[c, ft, hi], sib),
        ][k]
        return pltpu.make_async_remote_copy(src, dst, ag_s.at[s, lax.rem(c, 2), k], ag_r.at[s, c, k], device_id={"tp": dev})

    def rs(s, c, k, cut=None):
        col, got = (pl.ds(0, width), c) if cut is None else (pl.ds(*cut[:2]), n_chunks - 1 + cut[2])
        sent = (s, lax.rem(c, 2)) if cut is None or cut[2] == 0 else (0, cut[2] - 1)
        p, lo, hi = part(s, c), pl.ds(0, half), pl.ds(half, half)
        all_rows = pl.ds(0, blk)
        if k < 4:
            src, dst, dev = p.at[chips[k], 1 - core, all_rows, col], sbs[s].at[c, k, all_rows, col], sib
        else:
            src, dst, dev = [
                (p.at[far, core, lo, col], rbs[s].at[c, 0, pl.ds(0, half), col], right),
                (p.at[far, core, hi, col], rbs[s].at[c, 1, pl.ds(0, half), col], left),
                (p.at[right_chip, core, hi, col], fbs[s].at[c, 0, hi, col], right),
                (p.at[left_chip, core, lo, col], fbs[s].at[c, 1, lo, col], left),
                (p.at[right_chip, core, lo, col], fbs[s].at[c, 0, lo, col], right),
                (p.at[left_chip, core, hi, col], fbs[s].at[c, 1, hi, col], left),
            ][k - 4]
        return pltpu.make_async_remote_copy(src, dst, rs_s.at[*sent, k], rs_r.at[s, got, k], device_id={"tp": dev})

    def by_rows(rows, fn):
        def step(i, carry):
            fn(pl.ds(pl.multiple_of(i * SUB, SUB), SUB))
            return carry

        lax.fori_loop(0, rows // SUB, step, 0)

    def f32(v):
        return v.astype(F32)

    def row(v):
        return f32(v).reshape(1, v.shape[0])

    def normed(wide, gain):
        inv_rms = lax.rsqrt(jnp.mean(wide * wide, axis=-1, keepdims=True) + NORM_EPS)
        return (wide * inv_rms * row(gain[...])).astype(BF)

    def own_copy(s, c):
        slot = h_slot(s, c)
        return pltpu.make_async_copy(hbufs[s].at[slot], h_all[s].at[c, me], h_sem.at[s, slot])

    def x_copy(c):
        return pltpu.make_async_copy(x_hbm.at[c], xin, x_sem.at[0])

    def ag_send(s, c):
        own_copy(s, c).start()
        for k in (0, 2, 1, 3, 4):
            ag(s, c, k).start()

    def ag1_own(c):
        x_copy(c).wait()

        def fn(rows):
            hb1[h_slot(ATT, c), rows, :] = normed(f32(xin[rows, :]), g1_ref)

        by_rows(blk, fn)
        ag_send(ATT, c)

        @pl.when(c + 1 < n_chunks)
        def _():
            x_copy(c + 1).start()

    def ag_fwd(s, c):
        ag(s, c, 0).wait_recv()
        ag(s, c, 5).start()
        ag(s, c, 2).wait_recv()
        ag(s, c, 6).start()

    def ag_far(s, c):
        for got, send in ((1, 7), (3, 8), (5, 9), (6, 10)):
            ag(s, c, got).wait_recv()
            ag(s, c, send).start()

    def ag_fin(s, c):
        for k in (4, 7, 8, 9, 10):
            ag(s, c, k).wait_recv()
        for k in range(11):
            ag(s, c, k).wait_send()
        own_copy(s, c).wait()

    def rs_pair(s, c, cut=None):
        for k in range(4):
            rs(s, c, k, cut).start()

    def loads(srcs, cut):
        col, row_idx = (pl.ds(0, width), 0) if cut is None else (pl.ds(*cut[:2]), cut[2])
        return [pltpu.make_async_copy(src.at[:, col], dst.at[:, col], tmp_sem.at[row_idx, i]) for i, (src, dst) in enumerate(srcs)]

    lo_rows, hi_rows = pl.ds(0, half), pl.ds(half, half)

    def half_loads(s, c, cut):
        sb = sbs[s]
        return loads([(sb.at[c, 0], t_a), (sb.at[c, 1, hi_rows], t_b.at[hi_rows]), (sb.at[c, 2, lo_rows], t_b.at[lo_rows])], cut)

    def rs_half_load(s, c, cut=None):
        for k, cp in enumerate(half_loads(s, c, cut)):
            rs(s, c, k, cut).wait_recv()
            cp.start()

    def halves(fn):
        def step(i, carry):
            fn(pl.ds(pl.multiple_of(i * SUB, SUB), SUB), pl.ds(pl.multiple_of(half + i * SUB, SUB), SUB))
            return carry

        lax.fori_loop(0, half // SUB, step, 0)

    def rs_half(s, c, cut=None, eager=False):
        for cp in half_loads(s, c, cut):
            cp.wait()
        p, col = part(s, c), slice(None) if cut is None else pl.ds(*cut[:2])

        def fn(lo, hi):
            for rows in (lo, hi):
                p[far, core, rows, col] = (f32(p[far, core, rows, col]) + f32(t_a[rows, col])).astype(BF)
            p[right_chip, core, hi, col] = (f32(p[right_chip, core, hi, col]) + f32(t_b[hi, col])).astype(BF)
            p[left_chip, core, lo, col] = (f32(p[left_chip, core, lo, col]) + f32(t_b[lo, col])).astype(BF)

        halves(fn)
        for k in range(4, 8 if eager else 6):
            rs(s, c, k, cut).start()

    def relay_loads(s, c, cut):
        sb, rb = sbs[s], rbs[s]
        return loads(
            [(sb.at[c, 1, lo_rows], t_a.at[lo_rows]), (sb.at[c, 2, hi_rows], t_a.at[hi_rows]), (rb.at[c, 0], t_c.at[lo_rows]), (rb.at[c, 1], t_c.at[hi_rows])], cut
        )

    def rs_relay_load(s, c, cut=None):
        for k in (4, 5):
            rs(s, c, k, cut).wait_recv()
        for cp in relay_loads(s, c, cut):
            cp.start()

    def rs_relay(s, c, cut=None, eager=False):
        for cp in relay_loads(s, c, cut):
            cp.wait()
        p, col = part(s, c), slice(None) if cut is None else pl.ds(*cut[:2])

        def fn(lo, hi):
            p[right_chip, core, lo, col] = (f32(p[right_chip, core, lo, col]) + f32(t_a[lo, col]) + f32(t_c[lo, col])).astype(BF)
            p[left_chip, core, hi, col] = (f32(p[left_chip, core, hi, col]) + f32(t_a[hi, col]) + f32(t_c[hi, col])).astype(BF)

        halves(fn)
        for k in (8, 9) if eager else (8, 9, 6, 7):
            rs(s, c, k, cut).start()

    def fin_loads(s, c, cut):
        return loads([(sbs[s].at[c, 3], t_a), (fbs[s].at[c, 0], t_b), (fbs[s].at[c, 1], t_c)], cut)

    def rs_fin_load(s, c, cut=None):
        for k in (3, 6, 7, 8, 9):
            rs(s, c, k, cut).wait_recv()
        for cp in fin_loads(s, c, cut):
            cp.start()

    def rs_total(s, c, rows, col=slice(None)):
        p = part(s, c)
        return (f32(p[chip, core, rows, col]) + f32(t_a[rows, col]) + f32(t_b[rows, col]) + f32(t_c[rows, col])).astype(BF)

    def rs_sent(s, c, cut=None):
        for k in range(10):
            rs(s, c, k, cut).wait_send()

    def xmid_copy(c):
        return pltpu.make_async_copy(x_hbm.at[c], xmid, x_sem.at[1])

    def x1_store(c):
        return pltpu.make_async_copy(xmid, x1_hbm.at[c], st_sem.at[0])

    def xend_copy(c):
        return pltpu.make_async_copy(x1_hbm.at[c], xend, x_sem.at[2])

    def out_store(c):
        return pltpu.make_async_copy(xend, out_hbm.at[c], st_sem.at[1])

    def rs1_fin_load(c):
        @pl.when(c > 0)
        def _():
            x1_store(c - 1).wait()

        xmid_copy(c).start()
        rs_fin_load(ATT, c)

    def rs1_fin(c):
        for cp in fin_loads(ATT, c, None):
            cp.wait()
        xmid_copy(c).wait()

        def fn(rows):
            mid = (f32(xmid[rows, :]) + f32(rs_total(ATT, c, rows))).astype(BF)
            xmid[rows, :] = mid
            hb2[0, rows, :] = normed(f32(mid), g2_ref)

        by_rows(blk, fn)
        x1_store(c).start()
        ag_send(MLP, c)

    def rs2_fin_load(c):
        @pl.when(c > 0)
        def _():
            out_store(c - 1).wait()

        xend_copy(c).start()
        rs_fin_load(MLP, c)

    def rs2_add(c, cut=None):
        for cp in fin_loads(MLP, c, cut):
            cp.wait()
        col = slice(None) if cut is None else pl.ds(*cut[:2])

        def fn(rows):
            xend[rows, col] = (f32(xend[rows, col]) + f32(rs_total(MLP, c, rows, col))).astype(BF)

        by_rows(blk, fn)

    def rs2_fin(c):
        xend_copy(c).wait()
        rs2_add(c)
        out_store(c).start()
        rs_sent(MLP, c)

    def att_loads(a, r):
        return (
            pltpu.make_async_copy(h1_hbm.at[a, :, pl.ds(pl.multiple_of(r * half, half), half)], h1v, at_sem.at[0]),
            pltpu.make_async_copy(cs_hbm.at[a * R + r], csv, at_sem.at[3]),
        )

    def cache_loads(a, r):
        return (
            pltpu.make_async_copy(kc_hbm.at[a * R + r], kb, at_sem.at[1]),
            pltpu.make_async_copy(vc_hbm.at[a * R + r], vb, at_sem.at[2]),
        )

    def table(req, carry):
        pos = p_ref[req] + lax.broadcasted_iota(jnp.int32, (tokens, hd), 0)
        angles = f32(pos) * freq_ref[...]
        first = lax.broadcasted_iota(jnp.int32, (tokens, hd), 1) < hd // 2
        csv[...] = jnp.where(first, jnp.cos(angles), jnp.sin(angles))
        cp = pltpu.make_async_copy(csv, cs_hbm.at[req], at_sem.at[3])
        cp.start()
        cp.wait()
        return carry

    def attend(a, r):
        req = a * R + r
        p_out = part(ATT, a)
        for cp in (*att_loads(a, r), *cache_loads(a, r)):
            cp.wait()
        fresh = (r == 0) & ((a == 0) | (a >= LEAD))
        h = h1v[...].reshape(tokens, width)

        def project(cps, slot, bias):
            @pl.when(fresh)
            def _():
                for cp in cps:
                    cp.wait()

            total = jnp.dot(h, gu_buf[slot, :, 0 : bias.shape[1]], preferred_element_type=F32)
            return f32((total + bias).astype(BF))

        some_q = project(qa_loads(), 1, row(bq_ref[0:QA]))
        rest = project(qb_loads(), 0, jnp.concatenate([row(bq_ref[QA:qn]), row(bk_ref[...]), row(bv_ref[...])], axis=1))
        p, c = p_ref[req], c_ref[req]
        cs = csv[...]
        sc = pltpu.roll(cs, hd // 2, 1)
        first = lax.broadcasted_iota(jnp.int32, (tokens, hd), 1) < hd // 2
        cos, sin = jnp.where(first, cs, sc), jnp.where(first, -sc, cs)

        def head(j):
            return some_q[:, j * hd : (j + 1) * hd] if j * hd < QA else rest[:, j * hd - QA : (j + 1) * hd - QA]

        def rope(v):
            return v * cos + pltpu.roll(v, hd // 2, 1) * sin

        n_heads, groups = qn // hd, tokens // blk
        for j in range(n_heads):
            h2v[0:groups, :, j * hd : (j + 1) * hd] = rope(head(j)).astype(BF).reshape(groups, blk, hd)
        slot = lax.broadcasted_iota(jnp.int32, (slots, hd), 0)
        new = (slot >= p) & (slot < p + c)
        shift[slots : slots + tokens, :] = rope(head(n_heads))
        kb[...] = jnp.where(new, shift[pl.ds(slots - p, slots), :], f32(kb[...])).astype(BF)
        shift[slots : slots + tokens, :] = head(n_heads + 1)
        vb[...] = jnp.where(new, shift[pl.ds(slots - p, slots), :], f32(vb[...])).astype(BF)
        stores = (pltpu.make_async_copy(kb, ko_hbm.at[req], kv_sem.at[0]), pltpu.make_async_copy(vb, vo_hbm.at[req], kv_sem.at[1]))
        for cp in stores:
            cp.start()

        @pl.when(r + 1 < R)
        def _():
            for cp in att_loads(a, r + 1):
                cp.start()

        @pl.when((r == R - 1) & (a >= LEAD - 1))
        def _():
            start_gu()

        def scores(j):
            q = h2v[0:groups, :, j * hd : (j + 1) * hd].reshape(tokens, hd)
            return lax.dot_general(q, kb[...], (((1,), (1,)), ((), ())), preferred_element_type=F32)

        limit = p + jnp.minimum(lax.broadcasted_iota(jnp.int32, (tokens, slots), 0), c - 1)
        visible = lax.broadcasted_iota(jnp.int32, (tokens, slots), 1) <= limit
        sbuf[0] = scores(0)
        for j in range(n_heads):
            if j + 1 < n_heads:
                sbuf[(j + 1) % 2] = scores(j + 1)
            masked = jnp.where(visible, sbuf[j % 2], -1.0e30)
            expd = jnp.exp2((masked - jnp.max(masked, axis=1, keepdims=True)) * (hd**-0.5 * LOG2_E))
            probs = (expd * (1.0 / jnp.sum(expd, axis=1, keepdims=True))).astype(BF)
            mixed = jnp.dot(probs, vb[...], preferred_element_type=F32).astype(BF)
            h2v[groups : 2 * groups, :, j * hd : (j + 1) * hd] = mixed.reshape(groups, blk, hd)
        for cp in stores:
            cp.wait()

        @pl.when(r + 1 < R)
        def _():
            for cp in cache_loads(a, r + 1):
                cp.start()

        heads = h2v[groups : 2 * groups, :, 0:qn].reshape(tokens, qn)
        out = jnp.dot(heads, w_out[...], preferred_element_type=F32).astype(BF)
        p_out[:, :, pl.ds(pl.multiple_of(r * half, half), half), :] = out.reshape(n_chip, 2, half, width)

    def gu_copies(tile, slot):
        cols = pl.ds(pl.multiple_of(tile * GU, GU), GU)
        return (
            pltpu.make_async_copy(wg_hbm.at[:, cols], gu_buf.at[slot, :, pl.ds(0, GU)], gu_sem.at[slot, 0]),
            pltpu.make_async_copy(wu_hbm.at[:, cols], gu_buf.at[slot, :, pl.ds(GU, GU)], gu_sem.at[slot, 1]),
        )

    def dn_copy(tile, slot):
        cols = pl.ds(pl.multiple_of(tile * DN, DN), DN)
        return pltpu.make_async_copy(wd_hbm.at[:, cols], dn_buf.at[slot], dn_sem.at[slot])

    def h2_load(c):
        return pltpu.make_async_copy(h2_hbm.at[c], h2v, h2_sem)

    def start_gu():
        for tile in range(GU_SLOTS - 1):
            for cp in gu_copies(tile, tile):
                cp.start()

    def qa_loads():
        return (pltpu.make_async_copy(wq_hbm.at[:, pl.ds(0, QA)], gu_buf.at[1, :, pl.ds(0, QA)], w_sem.at[0]),)

    def qb_loads():
        left_q = qn - QA
        return (
            pltpu.make_async_copy(wq_hbm.at[:, pl.ds(QA, left_q)], gu_buf.at[0, :, pl.ds(0, left_q)], w_sem.at[1]),
            pltpu.make_async_copy(wk_hbm, gu_buf.at[0, :, pl.ds(left_q, hd)], w_sem.at[2]),
            pltpu.make_async_copy(wv_hbm, gu_buf.at[0, :, pl.ds(left_q + hd, hd)], w_sem.at[3]),
        )

    x_copy(0).start()
    barrier = pltpu.get_barrier_semaphore()
    for dev in (right, left, sib):
        pl.semaphore_signal(barrier, inc=1, device_id={"tp": dev})
    pl.semaphore_wait(barrier, 3)
    ag1_own(0)
    wo_copy = pltpu.make_async_copy(wo_hbm, w_out, w_sem.at[4])
    for cp in (*qa_loads(), *qb_loads(), wo_copy):
        cp.start()
    shift[...] = jnp.zeros_like(shift)
    lax.fori_loop(0, 2 * n_chunks * R // 3, table, 0)
    ag_fwd(ATT, 0)
    lax.fori_loop(2 * n_chunks * R // 3, n_chunks * R, table, 0)
    wo_copy.wait()

    def ready(c):
        ag_fin(ATT, c)
        for cp in (*att_loads(c, 0), *cache_loads(c, 0)):
            cp.start()

    def lead(i, carry):
        @pl.when(i == 0)
        def _():
            ag1_own(1)
            ag_far(ATT, 0)
            ready(0)

        @pl.when(i == 1)
        def _():
            ag_fwd(ATT, 1)
            ag1_own(2)

        @pl.when(i == R)
        def _():
            ag_far(ATT, 1)
            rs_pair(ATT, 0)
            ready(1)
            rs_half_load(ATT, 0)
            rs_half(ATT, 0, eager=True)

        @pl.when(i == R + 1)
        def _():
            rs_relay_load(ATT, 0)
            rs_relay(ATT, 0, eager=True)
            ag_fwd(ATT, 2)

        @pl.when(i == 2 * R)
        def _():
            rs_pair(ATT, 1)
            rs1_fin_load(0)
            rs1_fin(0)
            ag_far(ATT, 2)
            ready(2)
            rs_sent(ATT, 0)

        @pl.when(i == 2 * R + 1)
        def _():
            ag_fwd(MLP, 0)
            rs_half_load(ATT, 1)
            rs_half(ATT, 1)

        attend(lax.div(i, R), lax.rem(i, R))
        return carry

    lax.fori_loop(0, LEAD * R, lead, 0)
    ag_far(MLP, 0)
    rs_pair(ATT, 2)
    ag_fin(MLP, 0)
    h2_load(0).start()

    last = n_chunks - 1
    unit = (n_dn // DN_PARTS) * DN
    cuts = ((0, 2 * unit, 0), (2 * unit, 2 * unit, 1), (4 * unit, width - 4 * unit, 2))

    def gu_tile(j):
        slot = lax.rem(j, GU_SLOTS)

        @pl.when(j + GU_SLOTS - 1 < n_gu)
        def _():
            for cp in gu_copies(j + GU_SLOTS - 1, lax.rem(j + GU_SLOTS - 1, GU_SLOTS)):
                cp.start()

        for cp in gu_copies(j, slot):
            cp.wait()
        both = jnp.dot(h2v[...].reshape(n_dev * blk, width), gu_buf[slot], preferred_element_type=F32)
        gate, up = both[:, :GU], both[:, GU:]
        act[:, pl.ds(pl.multiple_of(j * GU, GU), GU)] = (jax.nn.silu(gate) * up).astype(BF)

    def dn_tile(s, j):
        slot = lax.rem(j, DN_SLOTS)

        @pl.when((s == last) & (j == n_dn - 1))
        def _():
            rs_relay_load(MLP, last, cuts[0])
            rs_half_load(MLP, last, cuts[1])
            rs_relay(MLP, last, cuts[0], True)
            rs_half(MLP, last, cuts[1], True)

        @pl.when(j + 1 < n_dn)
        def _():
            dn_copy(j + 1, 1 - slot).start()

        dn_copy(j, slot).wait()
        tile = jnp.dot(act[...], dn_buf[slot], preferred_element_type=F32).astype(BF)
        pp[p_slot(MLP, s), :, :, :, pl.ds(pl.multiple_of(j * DN, DN), DN)] = tile.reshape(n_chip, 2, blk, DN)

    def tiles(fn, part_idx, per):
        def one(i, carry):
            fn(part_idx * per + i)
            return carry

        lax.fori_loop(0, per, one, 0)

    def step(s, carry):
        nxt, att, old = s + 1, s + LEAD - 1, s - 1
        more = nxt < n_chunks
        has_att = (s > 0) & (att < n_chunks)

        def gu_part(k, carry):
            def at(when, cond, name, fn, chunk):
                @pl.when((k == when) & cond)
                def _():
                    fn(chunk)

            early, pen = s == 0, s == last - 1
            pick = lambda att_at, pen_at, else_at: jnp.where(has_att, att_at, jnp.where(pen, pen_at, else_at))
            at(0, pen, "rs1_relay", lambda c: rs_relay(ATT, c), nxt)
            at(2, s > 0, "rs2_half", lambda c: rs_half(MLP, c), old)
            at(jnp.where(early, 1, 3), s < last - 1, "rs1_relay", lambda c: rs_relay(ATT, c), nxt)
            at(8, pen, "ag2_fwd", lambda c: ag_fwd(MLP, c), nxt)
            at(pick(6, 8, 5), s > 0, "rs2_relay", lambda c: rs_relay(MLP, c), old)
            at(pick(-1, 5, 6), more, "rs1_fin", rs1_fin, nxt)
            at(1, s > 0, "rs2_half_load", lambda c: rs_half_load(MLP, c), old)
            at(1, has_att, "ag1_fwd", lambda c: ag_fwd(ATT, c), att)
            at(jnp.where(early, 0, 2), s < last - 1, "rs1_relay_load", lambda c: rs_relay_load(ATT, c), nxt)
            at(pick(5, 7, 4), s > 0, "rs2_relay_load", lambda c: rs_relay_load(MLP, c), old)
            at(6, has_att, "ag1_far", lambda c: ag_far(ATT, c), att)
            at(7, has_att, "ready", ready, att)
            at(pick(8, 4, 5), more, "rs1_fin_load", rs1_fin_load, nxt)

            @pl.when((k == GU_PARTS - 1) & has_att)
            def _():
                for cp in qa_loads():
                    cp.start()

            tiles(gu_tile, k, n_gu // GU_PARTS)
            return carry

        dn_copy(0, 0).start()
        h2_load(s).wait()
        lax.fori_loop(0, GU_PARTS, gu_part, 0)

        @pl.when(has_att)
        def _():
            for cp in qb_loads():
                cp.start()
            rs1_fin(nxt)

        @pl.when(more & jnp.logical_not(has_att))
        def _():
            start_gu()

        @pl.when(more)
        def _():
            rs_sent(ATT, nxt)

        def att_step(r, carry):
            @pl.when((r == R - 1) & has_att)
            def _():
                rs2_fin_load(old)

            @pl.when(has_att)
            def _():
                attend(att, r)

            return carry

        lax.fori_loop(0, R, att_step, 0)

        @pl.when(has_att)
        def _():
            rs_pair(ATT, att)
            rs2_fin(old)

        def dn_part(k, carry):
            def at(when, cond, name, fn, chunk):
                @pl.when((k == when) & cond)
                def _():
                    fn(chunk)

            pen = s == last - 1
            pick = lambda att_at, pen_at, else_at: jnp.where(has_att, att_at, jnp.where(pen, pen_at, else_at))

            def gathered(c):
                ag_fin(MLP, c)
                h2_load(c).start(priority=1)

            at(2, s == last, "rs2_fin", rs2_fin, old)
            at(2, att < n_chunks, "rs1_half", lambda c: rs_half(ATT, c), att)
            at(1, att < n_chunks, "rs1_half_load", lambda c: rs_half_load(ATT, c), att)
            at(0, more & jnp.logical_not(pen), "ag2_fwd", lambda c: ag_fwd(MLP, c), nxt)
            at(0, att + 1 < n_chunks, "ag1_own", ag1_own, att + 1)
            at(pick(3, 1, 2), more, "ag2_far", lambda c: ag_far(MLP, c), nxt)
            at(pick(4, 2, 4), more, "ag2_fin", gathered, nxt)
            at(4, s == last - 2, "rs1_relay_load", lambda c: rs_relay_load(ATT, c), att)
            at(jnp.where(pen, 4, 1), pen | (s == last), "rs2_fin_load", rs2_fin_load, old)
            at(2, s == last, "tail_pair", lambda c: rs_pair(MLP, c, cuts[0]), s)
            at(3, s == last, "tail_half_load", lambda c: rs_half_load(MLP, c, cuts[0]), s)
            at(3, s == last, "tail_half", lambda c: rs_half(MLP, c, cuts[0], True), s)
            at(4, s == last, "tail_pair", lambda c: rs_pair(MLP, c, cuts[1]), s)
            tiles(functools.partial(dn_tile, s), k, n_dn // DN_PARTS)
            return carry

        lax.fori_loop(0, DN_PARTS, dn_part, 0)

        @pl.when(s == last - 1)
        def _():
            rs2_fin(old)

        @pl.when(more)
        def _():
            rs_pair(MLP, s)

        return carry

    lax.fori_loop(0, n_chunks, step, 0)

    rs_pair(MLP, last, cuts[2])
    rs_half_load(MLP, last, cuts[2])
    rs_half(MLP, last, cuts[2], True)
    x1_store(last).wait()
    out_store(last - 1).wait()
    xend_copy(last).start()
    xend_copy(last).wait()
    rs_fin_load(MLP, last, cuts[0])
    rs_relay_load(MLP, last, cuts[1])
    rs_relay(MLP, last, cuts[1], True)
    rs2_add(last, cuts[0])
    rs_relay_load(MLP, last, cuts[2])
    rs_relay(MLP, last, cuts[2], True)
    for cut in cuts[1:]:
        rs_fin_load(MLP, last, cut)
        rs2_add(last, cut)
    out_store(last).start()
    for cut in cuts:
        rs_sent(MLP, last, cut)
    out_store(last).wait()


def hand_out(arrays):
    n_arrays, pieces = len(arrays), arrays[0].shape[0]
    per = [a.shape[0] // pieces for a in arrays]

    def kernel(*refs):
        srcs, dsts, bufs = (refs[i * n_arrays : (i + 1) * n_arrays] for i in range(len(refs) // n_arrays))
        got, put = refs[n_arrays * (len(refs) // n_arrays) :]
        order = [(i, j) for j in range(pieces) for i in range(n_arrays)]
        rows = lambda i, j: pl.ds(j * per[i], per[i])
        loads = [pltpu.make_async_copy(srcs[i].at[rows(i, j)], bufs[i].at[rows(i, j)], got.at[i, j]) for i, j in order]
        stores = [pltpu.make_async_copy(bufs[i].at[rows(i, j)], dsts[i].at[rows(i, j)], put.at[i, j]) for i, j in order]
        for cp in loads:
            cp.start()
        for load, store in zip(loads, stores):
            load.wait()
            store.start()
        for cp in stores:
            cp.wait()

    hbm = pl.BlockSpec(memory_space=pl.ANY)
    sems = pltpu.SemaphoreType.DMA((n_arrays, pieces))
    return pl.pallas_call(
        kernel,
        in_specs=[hbm] * n_arrays,
        out_specs=[hbm] * n_arrays,
        out_shape=[jax.ShapeDtypeStruct(a.shape, a.dtype) for a in arrays],
        scratch_shapes=[*[pltpu.VMEM(a.shape, a.dtype) for a in arrays], sems, sems],
        compiler_params=pltpu.CompilerParams(vmem_limit_bytes=67_000_000),
        name="post",
    )(*arrays)


def fused_layer(x, freq, b_q, b_k, b_v, k_cache, v_cache, prefix, valid, g_attn, g_mlp, w_q, w_k, w_v, w_o, w_gate, w_up, w_down, n_dev):
    n_req, rows, width = x.shape
    n_chunks, blk = n_req // R, R * rows
    slots, hd = k_cache.shape[1:]
    tokens, qn, ffn = n_dev * rows, w_q.shape[1], w_gate.shape[1]
    n_chip = n_dev // 2
    hbm, smem, vmem = (pl.BlockSpec(memory_space=m) for m in (pl.ANY, pltpu.SMEM, pltpu.VMEM))
    chunked = lambda *s: jax.ShapeDtypeStruct((n_chunks, *s, width), BF)
    out_shape = [
        chunked(blk),
        jax.ShapeDtypeStruct(k_cache.shape, BF),
        jax.ShapeDtypeStruct(v_cache.shape, BF),
        chunked(n_dev, blk),
        chunked(n_dev, blk),
        chunked(n_chip, blk),
        chunked(n_chip, blk),
        chunked(2, rows),
        chunked(2, rows),
        chunked(2, blk),
        chunked(2, blk),
        chunked(blk),
        jax.ShapeDtypeStruct((n_req, tokens, hd), F32),
    ]
    dma = lambda *s: pltpu.SemaphoreType.DMA(s)
    rows_buf = pltpu.VMEM((blk, width), BF)
    scratch = [
        pltpu.VMEM((qn, width), BF),
        pltpu.VMEM((GU_SLOTS, width, 2 * GU), BF),
        pltpu.VMEM((DN_SLOTS, ffn, DN), BF),
        pltpu.VMEM((n_dev, blk, width), BF),
        pltpu.VMEM((n_dev, rows, width), BF),
        pltpu.VMEM((n_dev * blk, ffn), BF),
        pltpu.VMEM((2, n_chip, 2, blk, width), BF),
        *[rows_buf] * 6,
        pltpu.VMEM((2, blk, width), BF),
        pltpu.VMEM((1, blk, width), BF),
        *[pltpu.VMEM((slots, hd), BF)] * 2,
        pltpu.VMEM((2 * slots, hd), F32),
        pltpu.VMEM((tokens, hd), F32),
        pltpu.VMEM((2, tokens, slots), F32),
        dma(2, 2, 11),
        dma(2, n_chunks, 11),
        dma(2, 2, 10),
        dma(2, n_chunks + 2, 10),
        dma(3, 4),
        dma(3),
        dma(2, 2),
        dma(2),
        dma(4),
        dma(2),
        dma(GU_SLOTS, 2),
        dma(DN_SLOTS),
        dma(5),
        pltpu.SemaphoreType.DMA,
    ]
    res = pl.pallas_call(
        layer_kernel,
        in_specs=[smem, smem] + [vmem] * 6 + [hbm] * 10,
        out_specs=[hbm] * len(out_shape),
        out_shape=out_shape,
        scratch_shapes=scratch,
        compiler_params=pltpu.CompilerParams(vmem_limit_bytes=67_000_000, collective_id=0, has_side_effects=True),
        name="layer",
    )(prefix, valid, b_q, b_k, b_v, g_attn, g_mlp, freq, x.reshape(n_chunks, blk, width), k_cache, v_cache, w_q, w_k, w_v, w_o, w_gate, w_up, w_down)
    out, k_out, v_out = hand_out(res[:3])
    return out.reshape(x.shape), k_out, v_out


def solution(mesh):
    row_spec = P("dp", "tp", None)
    cache_spec = P("dp", None, "tp", None)
    req_spec = P("dp")
    rep_spec = P(None)
    col_spec = P(None, "tp")
    bias_spec = P("tp")
    down_spec = P("tp", None)
    n_dev = mesh.shape["tp"]

    def layer(x_rows, k_cache, v_cache, prefix, valid, g_attn, w_q, b_q, w_k, b_k, w_v, b_v, w_o, g_mlp, w_gate, w_up, w_down):
        n_req, rows, _ = x_rows.shape
        slots, hd = k_cache.shape[1], k_cache.shape[3]
        keys, vals = k_cache.reshape(n_req, slots, hd), v_cache.reshape(n_req, slots, hd)
        inv_freq = ROPE_THETA ** (-np.arange(0, hd, 2) / hd)
        freq = jnp.asarray(np.tile(inv_freq, 2)[None], F32)
        out, k_out, v_out = fused_layer(x_rows, freq, b_q, b_k, b_v, keys, vals, prefix, valid, g_attn, g_mlp, w_q, w_k, w_v, w_o, w_gate, w_up, w_down, n_dev)
        return out, k_out.reshape(k_cache.shape), v_out.reshape(v_cache.shape)

    in_specs = (row_spec, cache_spec, cache_spec, req_spec, req_spec, rep_spec, col_spec, bias_spec, col_spec, bias_spec, col_spec, bias_spec, down_spec, rep_spec, col_spec, col_spec, down_spec)
    return jax.shard_map(layer, mesh=mesh, in_specs=in_specs, out_specs=(row_spec, cache_spec, cache_spec), check_vma=False)
```
